128 devices in a mesh: section: 2 (over z_lo), span: 32 (over x, y, core), seq: 2 (over z_hi).
Axes of the slice: x: 4, y: 4, z: 4 (z_hi: 2, z_lo: 2; z = z_hi * 2 + z_lo), core: 2. Of those that a mesh axis runs over, the one named last changes fastest.
Arguments:
- latents: bfloat16 [32256, 5120], P(('span', 'seq')), may hold values from -6 to 6
- queries: bfloat16 [2, 32256, 5120], P('section', ('span', 'seq')), may hold values from -12 to 12, as said below
- key_states: bfloat16 [2, 32256, 5120], P('section', ('span', 'seq')), may hold values from -12 to 12
- value_states: bfloat16 [2, 32256, 5120], P('section', ('span', 'seq')), may hold values from -6 to 6
- gate_scales: float32 [2, 5120], P('section'), may hold values from 4 to 12
- window: int32 [31], replicated, may hold values from 1 to 10, 170 in all
- intersection: int32 [31], replicated, may hold values from 1 to 10, 170 in all
- blend_index: int32 [31, 10], replicated, may hold values from 0 to 7
Outputs:
- denoised: bfloat16 [32256, 5120], P('span', ('section', 'seq'))
The draws below stay inside these ranges and needn't reach their ends.
Inputs may be any that keep to these rules, and one draw needn't show every extreme that they name: `queries`: queries of the span lie in the stated range. `window`: 10 is reached in every draw. `intersection`: 10 is reached in every draw.
All inputs are finite; a program needn't handle non-finite values.
Results may differ from the reference program's by a relative error of at most 0.0095.
Values may be sent and summed in bfloat16 or wider, within the bound.
No kernel may reach another device: no remote copies, remote signals or barrier semaphores. Data moves between devices by JAX's collectives and lax.ppermute only.
A program may use at most 192 MiB of HBM per device.

```python
import math
import jax
import jax.numpy as jnp
import numpy as np
from jax import lax

D = 5120
HEADS = 40
HEAD_DIM = 128
FRAMES = 21
TOK_FRAME = 48
BF = 10
WEIGHTS = 8
LAYERS = 2
SPANS = 32
PAIRS = 31
TOKENS = 32256


def draw_queries(key, part):
    base = jnp.clip(1.2 * jax.random.normal(jax.random.fold_in(key, 1), (LAYERS, TOKENS, D), jnp.float32), -12.0, 12.0)
    return base.astype(jnp.bfloat16)


def draw_key_states(key, part):
    base = jnp.clip(1.2 * jax.random.normal(jax.random.fold_in(key, 2), (LAYERS, TOKENS, D), jnp.float32), -12.0, 12.0)
    return base.astype(jnp.bfloat16)


def touch_ends(entries, stream_key, low, largest):
    index_at = [jax.random.randint(jax.random.fold_in(stream_key, axis), (), 0, length) for axis, length in enumerate(entries.shape)]
    widest = entries.shape.index(max(entries.shape))
    beside = index_at[:widest] + [(index_at[widest] + 1) % entries.shape[widest]] + index_at[widest + 1:]
    return entries.at[tuple(index_at)].set(low).at[tuple(beside)].set(largest)


def shard_levels(rng, dims, split, smallest, high):
    def one(dim, blocks):
        draws = jax.random.uniform(jax.random.fold_in(jax.random.fold_in(rng, 6), dim), (blocks,), jnp.float32, smallest / len(split), high / len(split))
        return jnp.repeat(jnp.exp(draws), dims[dim] // blocks).reshape((-1,) + (1,) * (len(dims) - dim - 1))

    loudness = one(*split[0])
    for cut in split[1:]:
        loudness = loudness * one(*cut)
    return loudness


def profile(number_of, total, bound, skew):
    portions = [(1 << 20) // math.isqrt(grade ** skew) + 1 for grade in range(2, number_of + 1)]
    rest, holding = total - bound - (number_of - 1), [1] * (number_of - 1)
    while rest > 0:
        movable = [i for i in range(number_of - 1) if holding[i] < bound]
        whole, left = sum([portions[i] for i in movable]), rest
        for i in movable:
            more = min(bound - holding[i], max(1, left * portions[i] // whole), rest)
            holding[i] = holding[i] + more
            rest = rest - more
    return np.array([bound] + holding)


def uneven(rng, number_of, total, reach, slope):
    if number_of == 2:
        one = jax.random.randint(rng, (), max(1, total - reach), min(reach, total - 1) + 1)
        return jnp.stack([one, total - one])
    sizes = jnp.asarray(profile(number_of, total, reach, slope), jnp.int32)
    twos = (number_of - 1) // 2
    source_of, receiver = sizes[1:1 + 2 * twos:2], sizes[2:2 + 2 * twos:2]
    margin = jnp.minimum(source_of - 1, reach - receiver)
    passed = jax.random.randint(jax.random.fold_in(rng, 1), (twos,), 0, 1 << 20) % (margin + 1)
    sizes = sizes.at[1:1 + 2 * twos:2].set(source_of - passed).at[2:2 + 2 * twos:2].set(receiver + passed)
    return sizes[jax.random.permutation(jax.random.fold_in(rng, 2), number_of)]


def scatter_about(stream_key, dims, scale, reach, pieces=(), kind=jnp.bfloat16):
    entries = scale * jax.random.normal(stream_key, dims, jnp.float32)
    if pieces:
        entries = entries * shard_levels(stream_key, dims, pieces, -0.22, 0.18)
    return jnp.clip(entries, -reach, reach).astype(kind)


def setup_inputs(seed: int = 0) -> dict:
    keys = jax.random.split(jax.random.key(seed), 9)
    return {
        "latents": scatter_about(keys[0], (TOKENS, D), 1.0, 6.0, ((0, 64),)),
        "queries": draw_queries(jax.random.fold_in(keys[8], 71), 0),
        "key_states": draw_key_states(jax.random.fold_in(keys[8], 71), 0),
        "value_states": scatter_about(keys[3], (LAYERS, TOKENS, D), 1.0, 6.0, ((0, 2), (1, 64))),
        "gate_scales": jnp.clip(jnp.exp(math.log(12.0) - 1.0986123 * jax.random.uniform(keys[4], (LAYERS, D), jnp.float32) ** shard_levels(keys[4], (LAYERS, D), ((0, 2),), -0.2, 0.2)), 4.0, 12.0),
        "window": uneven(keys[5], PAIRS, (BF + 1) * PAIRS // 2, BF, 1).astype(jnp.int32),
        "intersection": uneven(keys[6], PAIRS, (BF + 1) * PAIRS // 2, BF, 1).astype(jnp.int32),
        "blend_index": touch_ends(jax.random.randint(keys[7], (PAIRS, BF), 0, WEIGHTS), jax.random.fold_in(keys[7], 1), 0, WEIGHTS - 1).astype(jnp.int32),
    }


def attend_layer(query_all, key_all, value_all, window):
    span_tokens = FRAMES * TOK_FRAME
    tail_rows = BF * TOK_FRAME
    query_spans = query_all.reshape(SPANS, span_tokens, D)
    key_spans = key_all.reshape(SPANS, span_tokens, D)
    value_spans = value_all.reshape(SPANS, span_tokens, D)
    empty = jnp.zeros((1, tail_rows, D), key_all.dtype)
    prev_keys = jnp.concatenate([empty, key_spans[:-1, span_tokens - tail_rows:]], 0)
    prev_values = jnp.concatenate([empty, value_spans[:-1, span_tokens - tail_rows:]], 0)
    reach_all = jnp.concatenate([jnp.zeros((1,), jnp.int32), window.astype(jnp.int32)])

    def per_span(packed):
        query_block, key_block, value_block, key_tail, value_tail, reach_frames = packed
        key_full = jnp.concatenate([key_block, key_tail], 0)
        value_full = jnp.concatenate([value_block, value_tail], 0)
        frame_of = jnp.arange(tail_rows) // TOK_FRAME
        usable = jnp.concatenate([jnp.ones((span_tokens,), bool), frame_of >= BF - reach_frames])
        query_heads = query_block.astype(jnp.float32).reshape(span_tokens, HEADS, HEAD_DIM)
        key_heads = key_full.astype(jnp.float32).reshape(-1, HEADS, HEAD_DIM)
        value_heads = value_full.astype(jnp.float32).reshape(-1, HEADS, HEAD_DIM)
        scores = jnp.einsum('qhd,khd->hqk', query_heads, key_heads) * (1.0 / math.sqrt(HEAD_DIM))
        scores = jnp.where(usable[None, None, :], scores, -jnp.inf)
        row_max = lax.optimization_barrier(jnp.max(scores, axis=-1, keepdims=True))
        lifted = jnp.exp(scores - row_max)
        weights = (lifted / lax.optimization_barrier(jnp.sum(lifted, axis=-1, keepdims=True))).astype(jnp.bfloat16).astype(jnp.float32)
        combined = jnp.einsum('hqk,khd->qhd', weights, value_heads)
        return combined.reshape(span_tokens, D).astype(jnp.bfloat16)
    result = lax.map(per_span, (query_spans, key_spans, value_spans, prev_keys, prev_values, reach_all))
    return result.reshape(TOKENS, D)

def reference(latents, queries, key_states, value_states, gate_scales, window, intersection, blend_index):
    attended_zero = attend_layer(queries[0], key_states[0], value_states[0], window)
    attended_one = attend_layer(queries[1], key_states[1], value_states[1], window)
    after_one = (latents.astype(jnp.float32) + gate_scales[0] * attended_zero.astype(jnp.float32)).astype(jnp.bfloat16)
    second = (after_one.astype(jnp.float32) + gate_scales[1] * attended_one.astype(jnp.float32)).astype(jnp.bfloat16)
    grid = second.reshape(SPANS, FRAMES, TOK_FRAME, D)
    prev_tail = grid[:-1, FRAMES - BF:]
    frame_ids = jnp.arange(BF)
    source = jnp.clip(BF - intersection[:, None] + frame_ids[None, :], 0, BF - 1).astype(jnp.int32)
    picked = jax.vmap(lambda tail_block, picks: jnp.take(tail_block, picks, axis=0))(prev_tail, source)
    picked = picked.astype(jnp.float32)
    weight = ((blend_index.astype(jnp.float32) + 0.5) / WEIGHTS)[:, :, None, None]
    leading = grid[1:, :BF].astype(jnp.float32)
    active = (frame_ids[None, :] < intersection[:, None])[:, :, None, None]
    blended = jnp.where(active, weight * leading + (1.0 - weight) * picked, leading).astype(jnp.bfloat16)
    grid = grid.at[1:, :BF].set(blended)
    return grid.reshape(TOKENS, D)
```

```python
import functools
import math

import jax
import jax.numpy as jnp
from jax import lax
from jax.experimental import pallas as pl
from jax.experimental.pallas import tpu as pltpu
from jax.sharding import PartitionSpec as P

HEADS = 40
HEAD_DIM = 128
TOK_FRAME = 48
BF = 10
WEIGHTS = 8
TAIL = BF * TOK_FRAME
QUARTER_HEADS = 10
CHUNKS = (4, 3, 2, 1)
PAIR_AXES = ("section", "seq")


def spot(section, seq):
    return section * 2 + seq


def to_partner(block, flip_section, flip_seq):
    pairs = [
        (spot(s, q), spot(s ^ flip_section, q ^ flip_seq)) for s in range(2) for q in range(2)
    ]
    return lax.ppermute(block, PAIR_AXES, pairs)


def to_next_span(block):
    length = lax.axis_size("span")
    return lax.ppermute(block, "span", [(i, i + 1) for i in range(length - 1)])


def pack_kernel(width, start, cols_ref, q_ref, k_ref, v_ref, *rest):
    outs, (stage, in_sems, out_sems) = rest[:3], rest[3:]
    copies = []
    for dest in range(3):
        col = pl.multiple_of(cols_ref[dest] + start, HEAD_DIM)
        for which, ref in enumerate((q_ref, k_ref, v_ref)):
            taken = pltpu.make_async_copy(
                ref.at[0, :, pl.ds(col, width)], stage.at[dest, which], in_sems.at[dest, which]
            )
            taken.start()
            copies.append((dest, which, taken))
    sent = []
    for dest, which, taken in copies:
        taken.wait()
        put = pltpu.make_async_copy(
            stage.at[dest, which], outs[dest].at[which], out_sems.at[dest, which]
        )
        put.start()
        sent.append(put)
    for put in sent:
        put.wait()


def pack(cols, queries, key_states, value_states, start, width):
    rows = queries.shape[1]
    shape = jax.ShapeDtypeStruct((3, rows, width), jnp.bfloat16)
    return pl.pallas_call(
        functools.partial(pack_kernel, width, start),
        grid_spec=pltpu.PrefetchScalarGridSpec(
            num_scalar_prefetch=1,
            grid=(),
            in_specs=[pl.BlockSpec(memory_space=pl.ANY)] * 3,
            out_specs=[pl.BlockSpec(memory_space=pl.ANY)] * 3,
            scratch_shapes=[
                pltpu.VMEM((3, 3, rows, width), jnp.bfloat16),
                pltpu.SemaphoreType.DMA((3, 3)),
                pltpu.SemaphoreType.DMA((3, 3)),
            ],
        ),
        out_shape=[shape] * 3,
        cost_estimate=pl.CostEstimate(
            flops=9 * rows * width * 8, bytes_accessed=36 * rows * width, transcendentals=0
        ),
        name="pack",
    )(cols, queries, key_states, value_states)


def attend_kernel(
    info_ref, q_ref, k_ref, v_ref, seq_ref, sec_ref, dia_ref, near_ref, out_ref, qs, ks, vs
):
    rows = q_ref.shape[1]
    qs[0] = q_ref[0]
    ks[0] = k_ref[0]
    vs[0] = v_ref[0]
    for slot, ref in ((1, seq_ref), (2, sec_ref), (3, dia_ref)):
        qs[slot] = ref[0]
        ks[slot] = ref[1]
        vs[slot] = ref[2]
    factor = math.log2(math.e) / math.sqrt(HEAD_DIM)
    closed = info_ref[0]

    def one(index, carry):
        layer = index // 2
        query = qs[index]
        scores = []
        for key in (ks[2 * layer], ks[2 * layer + 1], near_ref[2 * layer]):
            scores.append(
                lax.dot_general(
                    query, key, (((1,), (1,)), ((), ())), preferred_element_type=jnp.float32
                )
            )
        place = lax.broadcasted_iota(jnp.int32, (1, TAIL), 1)
        scores[2] = jnp.where(place >= closed, scores[2], -jnp.inf)
        top = functools.reduce(
            jnp.maximum, [jnp.max(part, axis=-1, keepdims=True) for part in scores]
        )
        total = jnp.zeros((rows, 1), jnp.float32)
        mixed = jnp.zeros((rows, HEAD_DIM), jnp.float32)
        values = (vs[2 * layer], vs[2 * layer + 1], near_ref[2 * layer + 1])
        for part, value in zip(scores, values):
            lifted = jnp.exp2((part - top) * factor)
            total = total + jnp.sum(lifted, axis=-1, keepdims=True)
            mixed = mixed + jnp.dot(
                lifted.astype(jnp.bfloat16), value, preferred_element_type=jnp.float32
            )
        out_ref[index] = (mixed / total).astype(jnp.bfloat16)
        return carry

    lax.fori_loop(0, 4, one, 0)


def attend(info, queries, key_states, value_states, seq_in, sec_in, dia_in, near, first, heads):
    rows = queries.shape[1]
    keys = 2 * rows + TAIL
    local = pl.BlockSpec((1, rows, HEAD_DIM), lambda h, info: (0, 0, info[1] + first + h))
    partner = pl.BlockSpec((3, rows, HEAD_DIM), lambda h, info: (0, 0, h))
    return pl.pallas_call(
        attend_kernel,
        grid_spec=pltpu.PrefetchScalarGridSpec(
            num_scalar_prefetch=1,
            grid=(heads,),
            in_specs=[local, local, local, partner, partner, partner]
            + [pl.BlockSpec((4, TAIL, HEAD_DIM), lambda h, info: (0, 0, h))],
            out_specs=pl.BlockSpec((4, rows, HEAD_DIM), lambda h, info: (0, 0, h)),
            scratch_shapes=[pltpu.VMEM((4, rows, HEAD_DIM), jnp.bfloat16)] * 3,
        ),
        out_shape=jax.ShapeDtypeStruct((4, rows, heads * HEAD_DIM), jnp.bfloat16),
        cost_estimate=pl.CostEstimate(
            flops=heads * 4 * rows * keys * HEAD_DIM * 4,
            bytes_accessed=heads * HEAD_DIM * rows * 40,
            transcendentals=heads * 4 * rows * keys,
        ),
        compiler_params=pltpu.CompilerParams(vmem_limit_bytes=50 * 1024 * 1024),
        name="attend",
    )(info, queries, key_states, value_states, seq_in, sec_in, dia_in, near)


def combine_kernel(info_ref, att_ref, near_ref, far_ref, own_gate, other_gate, *rest):
    out_ref, tail_ref = rest[-2:]
    section, seq = info_ref[2], info_ref[3]
    rows = near_ref.shape[0]
    made = []
    for half, ref in enumerate((near_ref, far_ref)):
        own = own_gate[...] * att_ref[half].astype(jnp.float32)
        other = other_gate[...] * att_ref[2 + half].astype(jnp.float32)
        leads = section == 0
        first = jnp.where(leads, own, other)
        then = jnp.where(leads, other, own)
        after = (ref[...].astype(jnp.float32) + first).astype(jnp.bfloat16)
        made.append(after.astype(jnp.float32) + then)
    out_ref[seq] = made[0].astype(jnp.bfloat16)
    out_ref[1 - seq] = made[1].astype(jnp.bfloat16)
    late = jnp.where(seq == 1, made[0], made[1])
    tail_ref[...] = late[rows - TAIL :].astype(jnp.bfloat16)


def combine(info, att, latents, far, gate, other_gate, first, heads, second):
    rows, width = att.shape[1], heads * HEAD_DIM
    here = lambda h, info: (0, info[1] + first + h)
    placed = pl.BlockSpec((2, rows, HEAD_DIM), lambda h, info: (0, 0, first + h))
    operands = [info, att, latents, far, gate, other_gate]
    in_specs = [
        pl.BlockSpec((4, rows, HEAD_DIM), lambda h, info: (0, 0, h)),
        pl.BlockSpec((rows, HEAD_DIM), here),
        pl.BlockSpec((rows, HEAD_DIM), lambda h, info: (0, h)),
        pl.BlockSpec((1, HEAD_DIM), here),
        pl.BlockSpec((1, HEAD_DIM), lambda h, info: (0, first + h)),
    ]
    aliases = {}
    if second is not None:
        aliases = {len(operands): 0}
        operands.append(second)
        in_specs.append(pl.BlockSpec(memory_space=pl.ANY))
    return pl.pallas_call(
        combine_kernel,
        grid_spec=pltpu.PrefetchScalarGridSpec(
            num_scalar_prefetch=1,
            grid=(heads,),
            in_specs=in_specs,
            out_specs=[placed, pl.BlockSpec((TAIL, HEAD_DIM), lambda h, info: (0, h))],
        ),
        out_shape=[
            jax.ShapeDtypeStruct((2, rows, QUARTER_HEADS * HEAD_DIM), jnp.bfloat16),
            jax.ShapeDtypeStruct((TAIL, width), jnp.bfloat16),
        ],
        input_output_aliases=aliases,
        cost_estimate=pl.CostEstimate(
            flops=rows * width * 200, bytes_accessed=rows * width * 18, transcendentals=0
        ),
        name="combine",
    )(*operands)


def blend_kernel(heads, info_ref, index_ref, lead_ref, tail_ref, out_ref):
    shared = info_ref[4]
    for frame in range(BF):
        source = jnp.clip(BF - shared + frame, 0, BF - 1)
        weight = (index_ref[frame].astype(jnp.float32) + 0.5) / WEIGHTS
        span = pl.ds(frame * TOK_FRAME, TOK_FRAME)
        lead = lead_ref[span, :].astype(jnp.float32)
        before = tail_ref[
            pl.ds(pl.multiple_of(source * TOK_FRAME, TOK_FRAME), TOK_FRAME), :
        ].astype(jnp.float32)
        mixed = weight * lead + (1.0 - weight) * before
        out_ref[span, :] = jnp.where(frame < shared, mixed, lead).astype(jnp.bfloat16)


def blend(info, picks, second, tail, first, heads):
    placed = pl.BlockSpec((TAIL, HEAD_DIM), lambda h, info, picks: (0, first + h))
    return pl.pallas_call(
        functools.partial(blend_kernel, heads),
        grid_spec=pltpu.PrefetchScalarGridSpec(
            num_scalar_prefetch=2,
            grid=(heads,),
            in_specs=[placed, pl.BlockSpec((TAIL, HEAD_DIM), lambda h, info, picks: (0, h))],
            out_specs=placed,
        ),
        out_shape=jax.ShapeDtypeStruct(second.shape, second.dtype),
        input_output_aliases={2: 0},
        cost_estimate=pl.CostEstimate(
            flops=TAIL * heads * 12800, bytes_accessed=TAIL * heads * 768, transcendentals=0
        ),
        name="blend",
    )(info, picks, second, tail)


def local(
    latents, queries, key_states, value_states, gate_scales, window, intersection, blend_index
):
    rows = latents.shape[0]
    quarter = QUARTER_HEADS * HEAD_DIM
    span_pos = lax.axis_index("span")
    section = lax.axis_index("section")
    seq = lax.axis_index("seq")
    earlier = jnp.maximum(span_pos - 1, 0)
    follows = span_pos > 0
    closed = jnp.where(follows, TAIL - TOK_FRAME * window[earlier], TAIL)
    shared = jnp.where(follows, intersection[earlier], 0)
    info = jnp.stack(
        [closed, spot(section, seq) * QUARTER_HEADS, section, seq, shared]
    ).astype(jnp.int32)
    picks = blend_index[earlier]
    cols = quarter * jnp.stack(
        [spot(section, 1 - seq), spot(1 - section, seq), spot(1 - section, 1 - seq)]
    ).astype(jnp.int32)

    starts = [sum(CHUNKS[:i]) for i in range(len(CHUNKS))]
    arrived = []
    for first, heads in zip(starts, CHUNKS):
        for_seq, for_sec, for_dia = pack(
            cols, queries, key_states, value_states, first * HEAD_DIM, heads * HEAD_DIM
        )
        arrived.append(
            (to_partner(for_seq, 0, 1), to_partner(for_sec, 1, 0), to_partner(for_dia, 1, 1))
        )
    far_latents = []
    for first, heads in zip(starts, CHUNKS):
        sent = lax.dynamic_slice_in_dim(
            latents, cols[2] + first * HEAD_DIM, heads * HEAD_DIM, 1
        )
        far_latents.append(to_partner(sent, 1, 1))
    other_gate = to_partner(
        lax.dynamic_slice_in_dim(gate_scales, cols[1], quarter, 1), 1, 0
    )

    attended = []
    base = spot(section, seq) * quarter
    cut = rows - TAIL
    for (first, heads), (seq_in, sec_in, dia_in) in zip(zip(starts, CHUNKS), arrived):
        near = []
        for which, ref in ((1, key_states), (2, value_states)):
            mine = lax.dynamic_slice(
                ref, (0, cut, base + first * HEAD_DIM), (1, TAIL, heads * HEAD_DIM)
            )[0]
            near.append(jnp.where(seq == 1, mine, seq_in[which, cut:]))
        for which in (1, 2):
            near.append(jnp.where(seq == 1, sec_in[which, cut:], dia_in[which, cut:]))
        near = to_next_span(jnp.stack(near))
        attended.append(
            attend(
                info, queries, key_states, value_states, seq_in, sec_in, dia_in, near, first, heads
            )
        )

    second = None
    tails = []
    for (first, heads), att, far in zip(zip(starts, CHUNKS), attended, far_latents):
        second, tail = combine(
            info, att, latents, far, gate_scales, other_gate, first, heads, second
        )
        tails.append(to_next_span(tail))
    second = second.reshape(2 * rows, quarter)
    for (first, heads), tail in zip(zip(starts, CHUNKS), tails):
        second = blend(info, picks, second, tail, first, heads)
    return second


def solution(mesh):
    in_specs = (
        P(("span", "seq"), None),
        P("section", ("span", "seq"), None),
        P("section", ("span", "seq"), None),
        P("section", ("span", "seq"), None),
        P("section", None),
        P(),
        P(),
        P(),
    )
    out_specs = P("span", ("section", "seq"))
    return jax.shard_map(local, mesh=mesh, in_specs=in_specs, out_specs=out_specs, check_vma=False)
```

```python
import functools
import math

import jax
import jax.numpy as jnp
from jax import lax
from jax.experimental import pallas as pl
from jax.experimental.pallas import tpu as pltpu
from jax.sharding import PartitionSpec as P


HEAD_DIM = 128
TOK_FRAME = 48
BF = 10
WEIGHTS = 8
TAIL = BF * TOK_FRAME
QUARTER_HEADS = 10
CHUNKS = (2, 2, 2, 2, 1, 1)
GROUPS = ((0, 1), (2, 3), (4, 5))
VMEM_LIMIT = 66000 * 1024
PAIR_AXES = ("section", "seq")


def spot(section, seq):
    return section * 2 + seq


def to_partner(block, flip_section, flip_seq):
    pairs = [
        (spot(s, q), spot(s ^ flip_section, q ^ flip_seq)) for s in range(2) for q in range(2)
    ]
    return lax.ppermute(block, PAIR_AXES, pairs)


def to_next_span(block):
    length = lax.axis_size("span")
    return lax.ppermute(block, "span", [(i, i + 1) for i in range(length - 1)])


def pack_kernel(width, start, cols_ref, q_ref, k_ref, v_ref, *rest):
    outs, (stage, in_sems, out_sems) = rest[:3], rest[3:]
    copies = []
    for dest in range(3):
        col = pl.multiple_of(cols_ref[dest] + start, HEAD_DIM)
        for which, ref in enumerate((q_ref, k_ref, v_ref)):
            taken = pltpu.make_async_copy(
                ref.at[0, :, pl.ds(col, width)], stage.at[dest, which], in_sems.at[dest, which]
            )
            taken.start()
            copies.append((dest, which, taken))
    sent = []
    for dest, which, taken in copies:
        taken.wait()
        put = pltpu.make_async_copy(
            stage.at[dest, which], outs[dest].at[which], out_sems.at[dest, which]
        )
        put.start()
        sent.append(put)
    for put in sent:
        put.wait()


def pack(cols, queries, key_states, value_states, start, width):
    rows = queries.shape[1]
    shape = jax.ShapeDtypeStruct((3, rows, width), jnp.bfloat16)
    return pl.pallas_call(
        functools.partial(pack_kernel, width, start),
        grid_spec=pltpu.PrefetchScalarGridSpec(
            num_scalar_prefetch=1,
            grid=(),
            in_specs=[pl.BlockSpec(memory_space=pl.ANY)] * 3,
            out_specs=[pl.BlockSpec(memory_space=pl.ANY)] * 3,
            scratch_shapes=[
                pltpu.VMEM((3, 3, rows, width), jnp.bfloat16),
                pltpu.SemaphoreType.DMA((3, 3)),
                pltpu.SemaphoreType.DMA((3, 3)),
            ],
        ),
        out_shape=[shape] * 3,
        cost_estimate=pl.CostEstimate(
            flops=9 * rows * width * 8, bytes_accessed=36 * rows * width, transcendentals=0
        ),
        compiler_params=pltpu.CompilerParams(vmem_limit_bytes=VMEM_LIMIT),
        name="pack",
    )(cols, queries, key_states, value_states)


def near_kernel(
    width, start, info_ref, k_ref, v_ref, seq_ref, sec_ref, dia_ref, out_ref, stage, sems, out_sems
):
    rows = k_ref.shape[1]
    cut = pl.ds(rows - TAIL, TAIL)
    cols = pl.ds(pl.multiple_of(info_ref[1] * HEAD_DIM + start, HEAD_DIM), width)
    late = info_ref[3] == 1

    @pl.when(late)
    def _():
        pltpu.make_async_copy(k_ref.at[0, cut, cols], stage.at[0], sems.at[0]).start()
        pltpu.make_async_copy(v_ref.at[0, cut, cols], stage.at[1], sems.at[1]).start()
        pltpu.make_async_copy(sec_ref.at[1, cut], stage.at[2], sems.at[2]).start()
        pltpu.make_async_copy(sec_ref.at[2, cut], stage.at[3], sems.at[3]).start()

    @pl.when(jnp.logical_not(late))
    def _():
        pltpu.make_async_copy(seq_ref.at[1, cut], stage.at[0], sems.at[0]).start()
        pltpu.make_async_copy(seq_ref.at[2, cut], stage.at[1], sems.at[1]).start()
        pltpu.make_async_copy(dia_ref.at[1, cut], stage.at[2], sems.at[2]).start()
        pltpu.make_async_copy(dia_ref.at[2, cut], stage.at[3], sems.at[3]).start()

    for slot in range(4):
        pltpu.make_async_copy(seq_ref.at[1, cut], stage.at[slot], sems.at[slot]).wait()
        pltpu.make_async_copy(stage.at[slot], out_ref.at[slot], out_sems.at[slot]).start()
    for slot in range(4):
        pltpu.make_async_copy(stage.at[slot], out_ref.at[slot], out_sems.at[slot]).wait()


def near_rows(info, key_states, value_states, seq_in, sec_in, dia_in, start, width):
    return pl.pallas_call(
        functools.partial(near_kernel, width, start),
        grid_spec=pltpu.PrefetchScalarGridSpec(
            num_scalar_prefetch=1,
            grid=(),
            in_specs=[pl.BlockSpec(memory_space=pl.ANY)] * 5,
            out_specs=pl.BlockSpec(memory_space=pl.ANY),
            scratch_shapes=[
                pltpu.VMEM((4, TAIL, width), jnp.bfloat16),
                pltpu.SemaphoreType.DMA((4,)),
                pltpu.SemaphoreType.DMA((4,)),
            ],
        ),
        out_shape=jax.ShapeDtypeStruct((4, TAIL, width), jnp.bfloat16),
        cost_estimate=pl.CostEstimate(
            flops=4 * TAIL * width * 8, bytes_accessed=16 * TAIL * width, transcendentals=0
        ),
        compiler_params=pltpu.CompilerParams(vmem_limit_bytes=VMEM_LIMIT),
        name="near",
    )(info, key_states, value_states, seq_in, sec_in, dia_in)


def attend_kernel(
    info_ref, q_ref, k_ref, v_ref, seq_ref, sec_ref, dia_ref, near_ref, *rest
):
    out_ref, qs, ks, vs = rest[-4:]
    rows = q_ref.shape[1]

    @pl.when(pl.program_id(0) == 0)
    def _():
        lane = lax.broadcasted_iota(jnp.int32, (rows, HEAD_DIM), 1)
        for slot in range(6):
            vs[slot, :, HEAD_DIM:] = (lane == 0).astype(jnp.bfloat16)

    qs[0] = q_ref[0]
    ks[0] = k_ref[0]
    vs[0, :, :HEAD_DIM] = v_ref[0]
    for slot, ref in ((1, seq_ref), (2, sec_ref), (3, dia_ref)):
        qs[slot] = ref[0]
        ks[slot] = ref[1]
        vs[slot, :, :HEAD_DIM] = ref[2]
    vs[4, :TAIL, :HEAD_DIM] = near_ref[1]
    vs[5, :TAIL, :HEAD_DIM] = near_ref[3]
    factor = math.log2(math.e) / math.sqrt(HEAD_DIM)
    place = lax.broadcasted_iota(jnp.int32, (1, TAIL), 1)
    bias = jnp.where(place >= info_ref[0], 0.0, -jnp.inf)

    def one(layer, carry):
        keys = (ks[2 * layer], ks[2 * layer + 1], near_ref[2 * layer])
        values = (vs[2 * layer], vs[2 * layer + 1], vs[4 + layer, :TAIL])
        scores = []
        for half in range(2):
            query = qs[2 * layer + half]
            parts = [
                lax.dot_general(
                    query, key, (((1,), (1,)), ((), ())), preferred_element_type=jnp.float32
                )
                for key in keys
            ]
            scores.append(parts[:2] + [parts[2] + bias])
        lifted = []
        for parts in scores:
            top = factor * functools.reduce(
                jnp.maximum, [jnp.max(part, axis=-1, keepdims=True) for part in parts]
            )
            lifted.append([jnp.exp2(part * factor - top).astype(jnp.bfloat16) for part in parts])
        for half, parts in enumerate(lifted):
            mixed = sum(
                jnp.dot(part, value, preferred_element_type=jnp.float32)
                for part, value in zip(parts, values)
            )
            out_ref[2 * layer + half] = (
                mixed[:, :HEAD_DIM] / mixed[:, HEAD_DIM : HEAD_DIM + 1]
            ).astype(jnp.bfloat16)
        return carry

    lax.fori_loop(0, 2, one, 0)


def attend(
    info, queries, key_states, value_states, seq_in, sec_in, dia_in, near, first, heads, place,
    group_heads, filled,
):
    rows = queries.shape[1]
    keys = 2 * rows + TAIL
    local = pl.BlockSpec((1, rows, HEAD_DIM), lambda h, info: (0, 0, info[1] + first + h))
    partner = pl.BlockSpec((3, rows, HEAD_DIM), lambda h, info: (0, 0, h))
    operands = [info, queries, key_states, value_states, seq_in, sec_in, dia_in, near]
    in_specs = [local, local, local, partner, partner, partner]
    in_specs.append(pl.BlockSpec((4, TAIL, HEAD_DIM), lambda h, info: (0, 0, h)))
    aliases = {}
    if filled is not None:
        aliases = {len(operands): 0}
        operands.append(filled)
        in_specs.append(pl.BlockSpec(memory_space=pl.ANY))
    return pl.pallas_call(
        attend_kernel,
        grid_spec=pltpu.PrefetchScalarGridSpec(
            num_scalar_prefetch=1,
            grid=(heads,),
            in_specs=in_specs,
            out_specs=pl.BlockSpec((4, rows, HEAD_DIM), lambda h, info: (0, 0, place + h)),
            scratch_shapes=[pltpu.VMEM((4, rows, HEAD_DIM), jnp.bfloat16)] * 2
            + [pltpu.VMEM((6, rows, 2 * HEAD_DIM), jnp.bfloat16)],
        ),
        out_shape=jax.ShapeDtypeStruct((4, rows, group_heads * HEAD_DIM), jnp.bfloat16),
        input_output_aliases=aliases,
        cost_estimate=pl.CostEstimate(
            flops=heads * 4 * rows * keys * HEAD_DIM * 4,
            bytes_accessed=heads * HEAD_DIM * rows * 40,
            transcendentals=heads * 4 * rows * keys,
        ),
        compiler_params=pltpu.CompilerParams(vmem_limit_bytes=VMEM_LIMIT),
        name="attend",
    )(*operands)


def gated(info_ref, own_ref, other_ref, near_ref, far_ref, own_gate, other_gate, near):
    latent = jnp.where(near, near_ref[...], far_ref[...]).astype(jnp.float32)
    own = own_gate[...] * own_ref[0].astype(jnp.float32)
    other = other_gate[...] * other_ref[0].astype(jnp.float32)
    leads = info_ref[2] == 0
    after = (latent + jnp.where(leads, own, other)).astype(jnp.bfloat16)
    return after.astype(jnp.float32) + jnp.where(leads, other, own)


def late_kernel(info_ref, picks_ref, *rest):
    (own_ref, other_ref, near_ref, far_ref, own_gate, other_gate), rest = rest[:6], rest[6:]
    out_ref, tail_ref = rest[-2:]
    made = gated(
        info_ref, own_ref, other_ref, near_ref, far_ref, own_gate, other_gate, info_ref[3] == 1
    )
    out_ref[0] = made.astype(jnp.bfloat16)
    tail_ref[...] = made[made.shape[0] - TAIL :].astype(jnp.bfloat16)


def early_kernel(info_ref, picks_ref, *rest):
    (own_ref, other_ref, near_ref, far_ref, own_gate, other_gate, tail_ref), rest = (
        rest[:7], rest[7:]
    )
    out_ref = rest[-1]
    made = gated(
        info_ref, own_ref, other_ref, near_ref, far_ref, own_gate, other_gate, info_ref[3] == 0
    )
    out_ref[0] = made.astype(jnp.bfloat16)
    shared = info_ref[4]
    for frame in range(BF):
        source = jnp.clip(BF - shared + frame, 0, BF - 1)
        weight = (picks_ref[frame].astype(jnp.float32) + 0.5) / WEIGHTS
        begin = pl.multiple_of(source * TOK_FRAME, TOK_FRAME)
        before = tail_ref[pl.ds(begin, TOK_FRAME), :].astype(jnp.float32)
        lead = made[frame * TOK_FRAME : (frame + 1) * TOK_FRAME]
        lead = lead.astype(jnp.bfloat16).astype(jnp.float32)

        @pl.when(frame < shared)
        def _():
            mixed = weight * lead + (1.0 - weight) * before
            out_ref[0, pl.ds(frame * TOK_FRAME, TOK_FRAME), :] = mixed.astype(jnp.bfloat16)


def finish(late, info, picks, att, latents, far, gate, other_gate, first, heads, second, tail):
    rows = att.shape[1]
    width = 2 * HEAD_DIM
    half = 1 if late else 0
    from_own = lambda seq: jnp.where(seq == half, 0, 1)
    here = lambda h, info, picks: (0, info[1] // 2 + first // 2 + h)
    part = lambda h, info, picks: (0, h)
    operands = [info, picks, att, att, latents, far, gate, other_gate]
    in_specs = [
        pl.BlockSpec((1, rows, width), lambda h, info, picks: (from_own(info[3]), 0, h)),
        pl.BlockSpec((1, rows, width), lambda h, info, picks: (2 + from_own(info[3]), 0, h)),
        pl.BlockSpec((rows, width), here),
        pl.BlockSpec((rows, width), part),
        pl.BlockSpec((1, width), here),
        pl.BlockSpec((1, width), lambda h, info, picks: (0, first // 2 + h)),
    ]
    out_specs = [pl.BlockSpec((1, rows, width), lambda h, info, picks: (half, 0, first // 2 + h))]
    out_shape = [jax.ShapeDtypeStruct((2, rows, QUARTER_HEADS * HEAD_DIM), jnp.bfloat16)]
    if late:
        out_specs.append(pl.BlockSpec((TAIL, width), part))
        out_shape.append(jax.ShapeDtypeStruct((TAIL, heads * HEAD_DIM), jnp.bfloat16))
    else:
        operands.append(tail)
        in_specs.append(pl.BlockSpec((TAIL, width), part))
    aliases = {}
    if second is not None:
        aliases = {len(operands): 0}
        operands.append(second)
        in_specs.append(pl.BlockSpec(memory_space=pl.ANY))
    return pl.pallas_call(
        late_kernel if late else early_kernel,
        grid_spec=pltpu.PrefetchScalarGridSpec(
            num_scalar_prefetch=2,
            grid=(heads // 2,),
            in_specs=in_specs,
            out_specs=out_specs,
        ),
        out_shape=out_shape,
        input_output_aliases=aliases,
        cost_estimate=pl.CostEstimate(
            flops=rows * heads * HEAD_DIM * 200,
            bytes_accessed=rows * heads * HEAD_DIM * 12,
            transcendentals=0,
        ),
        compiler_params=pltpu.CompilerParams(vmem_limit_bytes=VMEM_LIMIT),
        name="late" if late else "early",
    )(*operands)


def local(
    latents, queries, key_states, value_states, gate_scales, window, intersection, blend_index
):
    rows = latents.shape[0]
    quarter = QUARTER_HEADS * HEAD_DIM
    span_pos = lax.axis_index("span")
    section = lax.axis_index("section")
    seq = lax.axis_index("seq")
    earlier = jnp.maximum(span_pos - 1, 0)
    follows = span_pos > 0
    closed = jnp.where(follows, TAIL - TOK_FRAME * window[earlier], TAIL)
    shared = jnp.where(follows, intersection[earlier], 0)
    info = jnp.stack(
        [closed, spot(section, seq) * QUARTER_HEADS, section, seq, shared]
    ).astype(jnp.int32)
    picks = blend_index[earlier]
    cols = quarter * jnp.stack(
        [spot(section, 1 - seq), spot(1 - section, seq), spot(1 - section, 1 - seq)]
    ).astype(jnp.int32)

    chunks = len(CHUNKS)
    starts = [sum(CHUNKS[:i]) for i in range(chunks)]
    other_gate = to_partner(
        lax.dynamic_slice_in_dim(gate_scales, cols[1], quarter, 1), 1, 0
    )
    arrived = []
    for first, heads in zip(starts, CHUNKS):
        for_seq, for_sec, for_dia = pack(
            cols, queries, key_states, value_states, first * HEAD_DIM, heads * HEAD_DIM
        )
        from_dia = to_partner(for_dia, 1, 1)
        from_seq = to_partner(for_seq, 0, 1)
        from_sec = to_partner(for_sec, 1, 0)
        arrived.append((from_seq, from_sec, from_dia))
    group_first = [starts[group[0]] for group in GROUPS]
    group_heads = [sum(CHUNKS[k] for k in group) for group in GROUPS]
    far_latents = []
    for first, heads in zip(group_first, group_heads):
        sent = lax.dynamic_slice_in_dim(
            latents, cols[2] + first * HEAD_DIM, heads * HEAD_DIM, 1
        )
        far_latents.append(to_partner(sent, 1, 1))

    attended = []
    for g, group in enumerate(GROUPS):
        filled = None
        for k in group:
            first, heads = starts[k], CHUNKS[k]
            near = near_rows(
                info, key_states, value_states, *arrived[k], first * HEAD_DIM,
                heads * HEAD_DIM,
            )
            near = to_next_span(near)
            filled = attend(
                info, queries, key_states, value_states, *arrived[k], near, first, heads,
                first - group_first[g], group_heads[g], filled,
            )
        attended.append(filled)

    tails = []

    def finished(second, g, late):
        return finish(
            late, info, picks, attended[g], latents, far_latents[g], gate_scales, other_gate,
            group_first[g], group_heads[g], second, None if late else tails[g],
        )

    second = None
    for g in range(len(GROUPS)):
        second, tail = finished(second, g, True)
        tails.append(to_next_span(tail))
    for g in range(len(GROUPS)):
        (second,) = finished(second, g, False)
    return second.reshape(2 * rows, quarter)


def solution(mesh):
    in_specs = (
        P(("span", "seq"), None),
        P("section", ("span", "seq"), None),
        P("section", ("span", "seq"), None),
        P("section", ("span", "seq"), None),
        P("section", None),
        P(),
        P(),
        P(),
    )
    out_specs = P("span", ("section", "seq"))

    return jax.shard_map(local, mesh=mesh, in_specs=in_specs, out_specs=out_specs, check_vma=False)
```

```python
import functools
import math

import jax
import jax.numpy as jnp
from jax import lax
from jax.experimental import pallas as pl
from jax.experimental.pallas import tpu as pltpu
from jax.sharding import PartitionSpec as P


HEAD_DIM = 128
TOK_FRAME = 48
BF = 10
WEIGHTS = 8
TAIL = BF * TOK_FRAME
QUARTER_HEADS = 10
CHUNKS = (3, 3, 2, 2)
GROUPS = ((0, 1), (2,), (3,))
SENDS = (("z", 0), ("z", 1), ("kv", 2), ("kv", 3), ("q", 2), ("q", 3))
VMEM_LIMIT = 66000 * 1024
PAIR_AXES = ("section", "seq")


def spot(section, seq):
    return section * 2 + seq


def to_partner(block, flip_section, flip_seq):
    pairs = [
        (spot(s, q), spot(s ^ flip_section, q ^ flip_seq)) for s in range(2) for q in range(2)
    ]
    return lax.ppermute(block, PAIR_AXES, pairs)


def to_next_span(block):
    length = lax.axis_size("span")
    return lax.ppermute(block, "span", [(i, i + 1) for i in range(length - 1)])


def pack_kernel(width, start, dests, count, *rest):
    sources, outs, (stage, in_sems, out_sems) = rest[:count], rest[count:-3], rest[-3:]
    section, seq = lax.axis_index("section"), lax.axis_index("seq")
    copies = []
    for at, (flip_section, flip_seq) in enumerate(dests):
        other_section = 1 - section if flip_section else section
        other_seq = 1 - seq if flip_seq else seq
        col = spot(other_section, other_seq) * QUARTER_HEADS * HEAD_DIM + start
        col = pl.multiple_of(col, HEAD_DIM)
        for which, ref in enumerate(sources):
            taken = pltpu.make_async_copy(
                ref.at[0, :, pl.ds(col, width)], stage.at[at, which], in_sems.at[at, which]
            )
            taken.start()
            copies.append((at, which, taken))
    sent = []
    for at, which, taken in copies:
        taken.wait()
        put = pltpu.make_async_copy(
            stage.at[at, which], outs[at].at[which], out_sems.at[at, which]
        )
        put.start()
        sent.append(put)
    for put in sent:
        put.wait()


def pack(sources, start, width, dests):
    rows, count = sources[0].shape[1], len(sources)
    shape = jax.ShapeDtypeStruct((count, rows, width), jnp.bfloat16)
    return pl.pallas_call(
        functools.partial(pack_kernel, width, start, dests, count),
        in_specs=[pl.BlockSpec(memory_space=pl.ANY)] * count,
        out_specs=[pl.BlockSpec(memory_space=pl.ANY)] * len(dests),
        scratch_shapes=[
            pltpu.VMEM((len(dests), count, rows, width), jnp.bfloat16),
            pltpu.SemaphoreType.DMA((len(dests), count)),
            pltpu.SemaphoreType.DMA((len(dests), count)),
        ],
        out_shape=[shape] * len(dests),
        cost_estimate=pl.CostEstimate(
            flops=count * len(dests) * rows * width * 8,
            bytes_accessed=4 * count * len(dests) * rows * width,
            transcendentals=0,
        ),
        compiler_params=pltpu.CompilerParams(vmem_limit_bytes=VMEM_LIMIT),
        name="pack",
    )(*sources)


def near_kernel(
    width, start, info_ref, k_ref, v_ref, seq_ref, sec_ref, dia_ref, out_ref, stage, sems, out_sems
):
    rows = k_ref.shape[1]
    cut = pl.ds(rows - TAIL, TAIL)
    cols = pl.ds(pl.multiple_of(info_ref[1] * HEAD_DIM + start, HEAD_DIM), width)
    late = info_ref[3] == 1

    @pl.when(late)
    def _():
        pltpu.make_async_copy(k_ref.at[0, cut, cols], stage.at[0], sems.at[0]).start()
        pltpu.make_async_copy(v_ref.at[0, cut, cols], stage.at[1], sems.at[1]).start()
        pltpu.make_async_copy(sec_ref.at[0, cut], stage.at[2], sems.at[2]).start()
        pltpu.make_async_copy(sec_ref.at[1, cut], stage.at[3], sems.at[3]).start()

    @pl.when(jnp.logical_not(late))
    def _():
        pltpu.make_async_copy(seq_ref.at[0, cut], stage.at[0], sems.at[0]).start()
        pltpu.make_async_copy(seq_ref.at[1, cut], stage.at[1], sems.at[1]).start()
        pltpu.make_async_copy(dia_ref.at[0, cut], stage.at[2], sems.at[2]).start()
        pltpu.make_async_copy(dia_ref.at[1, cut], stage.at[3], sems.at[3]).start()

    for slot in range(4):
        pltpu.make_async_copy(seq_ref.at[0, cut], stage.at[slot], sems.at[slot]).wait()
        pltpu.make_async_copy(stage.at[slot], out_ref.at[slot], out_sems.at[slot]).start()
    for slot in range(4):
        pltpu.make_async_copy(stage.at[slot], out_ref.at[slot], out_sems.at[slot]).wait()


def near_rows(info, key_states, value_states, seq_in, sec_in, dia_in, start, width):
    return pl.pallas_call(
        functools.partial(near_kernel, width, start),
        grid_spec=pltpu.PrefetchScalarGridSpec(
            num_scalar_prefetch=1,
            grid=(),
            in_specs=[pl.BlockSpec(memory_space=pl.ANY)] * 5,
            out_specs=pl.BlockSpec(memory_space=pl.ANY),
            scratch_shapes=[
                pltpu.VMEM((4, TAIL, width), jnp.bfloat16),
                pltpu.SemaphoreType.DMA((4,)),
                pltpu.SemaphoreType.DMA((4,)),
            ],
        ),
        out_shape=jax.ShapeDtypeStruct((4, TAIL, width), jnp.bfloat16),
        cost_estimate=pl.CostEstimate(
            flops=4 * TAIL * width * 8, bytes_accessed=16 * TAIL * width, transcendentals=0
        ),
        compiler_params=pltpu.CompilerParams(vmem_limit_bytes=VMEM_LIMIT),
        name="near",
    )(info, key_states, value_states, seq_in, sec_in, dia_in)


def attend_kernel(
    info_ref, q_ref, k_ref, v_ref, seq_q, sec_q, dia_q, seq_kv, sec_kv, dia_kv, near_ref,
    own_gate, other_gate, *rest
):
    out_ref, qs, ks, vs = rest[-4:]
    rows = q_ref.shape[1]

    @pl.when(pl.program_id(0) == 0)
    def _():
        lane = lax.broadcasted_iota(jnp.int32, (rows, HEAD_DIM), 1)
        for slot in range(6):
            vs[slot, :, HEAD_DIM:] = (lane == 0).astype(jnp.bfloat16)

    qs[0] = q_ref[0]
    ks[0] = k_ref[0]
    vs[0, :, :HEAD_DIM] = v_ref[0]
    for slot, q_in, kv_in in ((1, seq_q, seq_kv), (2, sec_q, sec_kv), (3, dia_q, dia_kv)):
        qs[slot] = q_in[0]
        ks[slot] = kv_in[0]
        vs[slot, :, :HEAD_DIM] = kv_in[1]
    vs[4, :TAIL, :HEAD_DIM] = near_ref[1]
    vs[5, :TAIL, :HEAD_DIM] = near_ref[3]
    factor = math.log2(math.e) / math.sqrt(HEAD_DIM)
    place = lax.broadcasted_iota(jnp.int32, (1, TAIL), 1)
    bias = jnp.where(place >= info_ref[0], 0.0, -jnp.inf)

    gated = [None, None]
    for layer, gate_ref in enumerate((own_gate, other_gate)):
        keys = (ks[2 * layer], ks[2 * layer + 1], near_ref[2 * layer])
        values = (vs[2 * layer], vs[2 * layer + 1], vs[4 + layer, :TAIL])
        scores = []
        for half in range(2):
            query = qs[2 * layer + half]
            parts = [
                lax.dot_general(
                    query, key, (((1,), (1,)), ((), ())), preferred_element_type=jnp.float32
                )
                for key in keys
            ]
            scores.append(parts[:2] + [parts[2] + bias])
        lifted = []
        for parts in scores:
            top = factor * functools.reduce(
                jnp.maximum, [jnp.max(part, axis=-1, keepdims=True) for part in parts]
            )
            lifted.append([jnp.exp2(part * factor - top).astype(jnp.bfloat16) for part in parts])
        for half, parts in enumerate(lifted):
            mixed = sum(
                jnp.dot(part, value, preferred_element_type=jnp.float32)
                for part, value in zip(parts, values)
            )
            attended = (mixed[:, :HEAD_DIM] / mixed[:, HEAD_DIM : HEAD_DIM + 1]).astype(
                jnp.bfloat16
            )
            term = gate_ref[...] * attended.astype(jnp.float32)
            if layer == 0:
                gated[half] = term
            else:
                out_ref[half] = (gated[half] + term).astype(jnp.bfloat16)


def attend(
    info, queries, key_states, value_states, queries_in, pairs_in, near, gate, other_gate, first,
    heads, place, group_heads, filled,
):
    rows = queries.shape[1]
    keys = 2 * rows + TAIL
    local = pl.BlockSpec((1, rows, HEAD_DIM), lambda h, info: (0, 0, info[1] + first + h))
    last = queries_in[0].shape[0] - 1
    operands = [info, queries, key_states, value_states, *queries_in, *pairs_in, near]
    operands += [gate, other_gate]
    in_specs = [local, local, local]
    in_specs += [pl.BlockSpec((1, rows, HEAD_DIM), lambda h, info: (last, 0, h))] * 3
    in_specs += [pl.BlockSpec((2, rows, HEAD_DIM), lambda h, info: (0, 0, h))] * 3
    in_specs.append(pl.BlockSpec((4, TAIL, HEAD_DIM), lambda h, info: (0, 0, h)))
    in_specs.append(pl.BlockSpec((1, HEAD_DIM), lambda h, info: (0, info[1] + first + h)))
    in_specs.append(pl.BlockSpec((1, HEAD_DIM), lambda h, info: (0, first + h)))
    aliases = {}
    if filled is not None:
        aliases = {len(operands): 0}
        operands.append(filled)
        in_specs.append(pl.BlockSpec(memory_space=pl.ANY))
    return pl.pallas_call(
        attend_kernel,
        grid_spec=pltpu.PrefetchScalarGridSpec(
            num_scalar_prefetch=1,
            grid=(heads,),
            in_specs=in_specs,
            out_specs=pl.BlockSpec((2, rows, HEAD_DIM), lambda h, info: (0, 0, place + h)),
            scratch_shapes=[pltpu.VMEM((4, rows, HEAD_DIM), jnp.bfloat16)] * 2
            + [pltpu.VMEM((6, rows, 2 * HEAD_DIM), jnp.bfloat16)],
        ),
        out_shape=jax.ShapeDtypeStruct((2, rows, group_heads * HEAD_DIM), jnp.bfloat16),
        input_output_aliases=aliases,
        cost_estimate=pl.CostEstimate(
            flops=heads * 4 * rows * keys * HEAD_DIM * 4,
            bytes_accessed=heads * HEAD_DIM * rows * 40,
            transcendentals=heads * 4 * rows * keys,
        ),
        compiler_params=pltpu.CompilerParams(vmem_limit_bytes=VMEM_LIMIT),
        name="attend",
    )(*operands)


def tail_rows(gated, latents, far, seq, first, width, base):
    cut = far.shape[0] - TAIL
    added = lax.dynamic_slice(gated, (1 - seq, cut, 0), (1, TAIL, width))[0]
    near = lax.dynamic_slice(latents, (cut, base + first * HEAD_DIM), (TAIL, width))
    latent = jnp.where(seq == 1, near, far[cut:])
    return (latent.astype(jnp.float32) + added.astype(jnp.float32)).astype(jnp.bfloat16)


def finish_kernel(info_ref, picks_ref, gated_ref, near_ref, far_ref, tail_ref, *rest):
    out_ref = rest[-1]
    seq = info_ref[3]
    for half, ref in enumerate((near_ref, far_ref)):
        whole = ref[...].astype(jnp.float32) + gated_ref[half].astype(jnp.float32)
        out_ref[seq if half == 0 else 1 - seq] = whole.astype(jnp.bfloat16)
    shared = info_ref[4]
    for frame in range(BF):
        source = jnp.clip(BF - shared + frame, 0, BF - 1)
        weight = (picks_ref[frame].astype(jnp.float32) + 0.5) / WEIGHTS
        begin = pl.multiple_of(source * TOK_FRAME, TOK_FRAME)
        place = pl.ds(frame * TOK_FRAME, TOK_FRAME)

        @pl.when(frame < shared)
        def _():
            before = tail_ref[pl.ds(begin, TOK_FRAME), :].astype(jnp.float32)
            lead = out_ref[0, place, :].astype(jnp.float32)
            mixed = weight * lead + (1.0 - weight) * before
            out_ref[0, place, :] = mixed.astype(jnp.bfloat16)


def finish(info, picks, gated, latents, far, tail, first, heads, second):
    rows = gated.shape[1]
    width = 2 * HEAD_DIM
    here = lambda h, info, picks: (0, info[1] // 2 + first // 2 + h)
    part = lambda h, info, picks: (0, h)
    operands = [info, picks, gated, latents, far, tail]
    in_specs = [
        pl.BlockSpec((2, rows, width), lambda h, info, picks: (0, 0, h)),
        pl.BlockSpec((rows, width), here),
        pl.BlockSpec((rows, width), part),
        pl.BlockSpec((TAIL, width), part),
    ]
    aliases = {}
    if second is not None:
        aliases = {len(operands): 0}
        operands.append(second)
        in_specs.append(pl.BlockSpec(memory_space=pl.ANY))
    return pl.pallas_call(
        finish_kernel,
        grid_spec=pltpu.PrefetchScalarGridSpec(
            num_scalar_prefetch=2,
            grid=(heads // 2,),
            in_specs=in_specs,
            out_specs=pl.BlockSpec(
                (2, rows, width), lambda h, info, picks: (0, 0, first // 2 + h)
            ),
        ),
        out_shape=jax.ShapeDtypeStruct((2, rows, QUARTER_HEADS * HEAD_DIM), jnp.bfloat16),
        input_output_aliases=aliases,
        cost_estimate=pl.CostEstimate(
            flops=rows * heads * HEAD_DIM * 200,
            bytes_accessed=rows * heads * HEAD_DIM * 18,
            transcendentals=0,
        ),
        compiler_params=pltpu.CompilerParams(vmem_limit_bytes=VMEM_LIMIT),
        name="finish",
    )(*operands)


def local(
    latents, queries, key_states, value_states, gate_scales, window, intersection, blend_index
):
    rows = latents.shape[0]
    quarter = QUARTER_HEADS * HEAD_DIM
    span_pos = lax.axis_index("span")
    section = lax.axis_index("section")
    seq = lax.axis_index("seq")
    earlier = jnp.maximum(span_pos - 1, 0)
    follows = span_pos > 0
    closed = jnp.where(follows, TAIL - TOK_FRAME * window[earlier], TAIL)
    shared = jnp.where(follows, intersection[earlier], 0)
    info = jnp.stack(
        [closed, spot(section, seq) * QUARTER_HEADS, section, seq, shared]
    ).astype(jnp.int32)
    picks = blend_index[earlier]
    base = spot(section, seq) * quarter
    far_base = spot(1 - section, 1 - seq) * quarter

    chunks, groups = len(CHUNKS), len(GROUPS)
    starts = [sum(CHUNKS[:i]) for i in range(chunks)]
    group_first = [starts[group[0]] for group in GROUPS]
    group_heads = [sum(CHUNKS[k] for k in group) for group in GROUPS]
    queries_in, pairs_in = {}, {}
    for kind, k in SENDS:
        first, heads = starts[k], CHUNKS[k]
        sources = {"z": (key_states, value_states, queries), "kv": (key_states, value_states),
                   "q": (queries,)}[kind]
        ways = {"dia": (1, 1), "seq": (0, 1), "sec": (1, 0)}
        arrived = {}
        batches = (("dia",), ("seq", "sec")) if (kind, k) == SENDS[0] else (tuple(ways),)
        for batch in batches:
            packed = pack(
                sources, first * HEAD_DIM, heads * HEAD_DIM, tuple(ways[way] for way in batch)
            )
            for way, block in zip(batch, packed):
                arrived[way] = to_partner(block, *ways[way])
        arrived = (arrived["seq"], arrived["sec"], arrived["dia"])
        if kind in ("z", "q"):
            queries_in[k] = arrived
        if kind in ("z", "kv"):
            pairs_in[k] = arrived
    far_latents = []
    for first, heads in zip(group_first, group_heads):
        sent = lax.dynamic_slice_in_dim(
            latents, far_base + first * HEAD_DIM, heads * HEAD_DIM, 1
        )
        far_latents.append(to_partner(sent, 1, 1))
    other_gate = to_partner(
        lax.dynamic_slice_in_dim(gate_scales, spot(1 - section, seq) * quarter, quarter, 1), 1, 0
    )

    attended = []
    for g, group in enumerate(GROUPS):
        filled = None
        for k in group:
            first, heads = starts[k], CHUNKS[k]
            near = near_rows(
                info, key_states, value_states, *pairs_in[k], first * HEAD_DIM,
                heads * HEAD_DIM,
            )
            near = to_next_span(near)
            filled = attend(
                info, queries, key_states, value_states, queries_in[k], pairs_in[k], near,
                gate_scales, other_gate, first, heads, first - group_first[g], group_heads[g], filled,
            )
        attended.append(filled)

    tails = []
    for g in range(groups):
        far = far_latents[g]
        if g:
            far, _ = lax.optimization_barrier((far, tails[-1]))
        tail = tail_rows(
            attended[g], latents, far, seq, group_first[g], group_heads[g] * HEAD_DIM, base
        )
        tails.append(tail)
    arrived_tails = []
    for g in range(groups):
        arrived_tails.append(to_next_span(tails[g]))
    second = None
    for g in range(groups):
        second = finish(
            info, picks, attended[g], latents, far_latents[g], arrived_tails[g],
            group_first[g], group_heads[g], second,
        )
    return second.reshape(2 * rows, quarter)


def solution(mesh):
    in_specs = (
        P(("span", "seq"), None),
        P("section", ("span", "seq"), None),
        P("section", ("span", "seq"), None),
        P("section", ("span", "seq"), None),
        P("section", None),
        P(),
        P(),
        P(),
    )
    out_specs = P("span", ("section", "seq"))

    return jax.shard_map(local, mesh=mesh, in_specs=in_specs, out_specs=out_specs, check_vma=False)
```

```python
import functools
import math

import jax
import jax.numpy as jnp
from jax import lax
from jax.experimental import pallas as pl
from jax.experimental.pallas import tpu as pltpu
from jax.sharding import PartitionSpec as P


HEAD_DIM = 128
TOK_FRAME = 48
BF = 10
WEIGHTS = 8
TAIL = BF * TOK_FRAME
QUARTER_HEADS = 10
CHUNKS = (3, 3, 2, 2)
GROUPS = ((0, 1), (2,), (3,))
FINISHES = ((0,), (1, 2))
SENDS = (("z", 0), ("z", 1), ("kv", 2), ("kv", 3), ("q", 2), ("q", 3))
VMEM_LIMIT = 66000 * 1024
PAIR_AXES = ("section", "seq")


def spot(section, seq):
    return section * 2 + seq


def to_partner(block, flip_section, flip_seq):
    pairs = [
        (spot(s, q), spot(s ^ flip_section, q ^ flip_seq)) for s in range(2) for q in range(2)
    ]
    return lax.ppermute(block, PAIR_AXES, pairs)


def to_next_span(block):
    length = lax.axis_size("span")
    return lax.ppermute(block, "span", [(i, i + 1) for i in range(length - 1)])


def pack_kernel(width, start, dests, count, *rest):
    sources, outs, (stage, in_sems, out_sems) = rest[:count], rest[count:-3], rest[-3:]
    section, seq = lax.axis_index("section"), lax.axis_index("seq")
    copies = []
    for at, (flip_section, flip_seq) in enumerate(dests):
        other_section = 1 - section if flip_section else section
        other_seq = 1 - seq if flip_seq else seq
        col = spot(other_section, other_seq) * QUARTER_HEADS * HEAD_DIM + start
        col = pl.multiple_of(col, HEAD_DIM)
        for which, ref in enumerate(sources):
            taken = pltpu.make_async_copy(
                ref.at[0, :, pl.ds(col, width)], stage.at[at, which], in_sems.at[at, which]
            )
            taken.start()
            copies.append((at, which, taken))
    sent = []
    for at, which, taken in copies:
        taken.wait()
        put = pltpu.make_async_copy(
            stage.at[at, which], outs[at].at[which], out_sems.at[at, which]
        )
        put.start()
        sent.append(put)
    for put in sent:
        put.wait()


def pack(sources, start, width, dests):
    rows, count = sources[0].shape[1], len(sources)
    shape = jax.ShapeDtypeStruct((count, rows, width), jnp.bfloat16)
    return pl.pallas_call(
        functools.partial(pack_kernel, width, start, dests, count),
        in_specs=[pl.BlockSpec(memory_space=pl.ANY)] * count,
        out_specs=[pl.BlockSpec(memory_space=pl.ANY)] * len(dests),
        scratch_shapes=[
            pltpu.VMEM((len(dests), count, rows, width), jnp.bfloat16),
            pltpu.SemaphoreType.DMA((len(dests), count)),
            pltpu.SemaphoreType.DMA((len(dests), count)),
        ],
        out_shape=[shape] * len(dests),
        cost_estimate=pl.CostEstimate(
            flops=count * len(dests) * rows * width * 8,
            bytes_accessed=4 * count * len(dests) * rows * width,
            transcendentals=0,
        ),
        compiler_params=pltpu.CompilerParams(vmem_limit_bytes=VMEM_LIMIT),
        name="pack",
    )(*sources)


def near_kernel(
    width, start, info_ref, k_ref, v_ref, seq_ref, sec_ref, dia_ref, out_ref, stage, sems, out_sems
):
    rows = k_ref.shape[1]
    cut = pl.ds(rows - TAIL, TAIL)
    cols = pl.ds(pl.multiple_of(info_ref[1] * HEAD_DIM + start, HEAD_DIM), width)
    late = info_ref[3] == 1

    @pl.when(late)
    def _():
        pltpu.make_async_copy(k_ref.at[0, cut, cols], stage.at[0], sems.at[0]).start()
        pltpu.make_async_copy(v_ref.at[0, cut, cols], stage.at[1], sems.at[1]).start()
        pltpu.make_async_copy(sec_ref.at[0, cut], stage.at[2], sems.at[2]).start()
        pltpu.make_async_copy(sec_ref.at[1, cut], stage.at[3], sems.at[3]).start()

    @pl.when(jnp.logical_not(late))
    def _():
        pltpu.make_async_copy(seq_ref.at[0, cut], stage.at[0], sems.at[0]).start()
        pltpu.make_async_copy(seq_ref.at[1, cut], stage.at[1], sems.at[1]).start()
        pltpu.make_async_copy(dia_ref.at[0, cut], stage.at[2], sems.at[2]).start()
        pltpu.make_async_copy(dia_ref.at[1, cut], stage.at[3], sems.at[3]).start()

    for slot in range(4):
        pltpu.make_async_copy(seq_ref.at[0, cut], stage.at[slot], sems.at[slot]).wait()
        pltpu.make_async_copy(stage.at[slot], out_ref.at[slot], out_sems.at[slot]).start()
    for slot in range(4):
        pltpu.make_async_copy(stage.at[slot], out_ref.at[slot], out_sems.at[slot]).wait()


def near_rows(info, key_states, value_states, seq_in, sec_in, dia_in, start, width):
    return pl.pallas_call(
        functools.partial(near_kernel, width, start),
        grid_spec=pltpu.PrefetchScalarGridSpec(
            num_scalar_prefetch=1,
            grid=(),
            in_specs=[pl.BlockSpec(memory_space=pl.ANY)] * 5,
            out_specs=pl.BlockSpec(memory_space=pl.ANY),
            scratch_shapes=[
                pltpu.VMEM((4, TAIL, width), jnp.bfloat16),
                pltpu.SemaphoreType.DMA((4,)),
                pltpu.SemaphoreType.DMA((4,)),
            ],
        ),
        out_shape=jax.ShapeDtypeStruct((4, TAIL, width), jnp.bfloat16),
        cost_estimate=pl.CostEstimate(
            flops=4 * TAIL * width * 8, bytes_accessed=16 * TAIL * width, transcendentals=0
        ),
        compiler_params=pltpu.CompilerParams(vmem_limit_bytes=VMEM_LIMIT),
        name="near",
    )(info, key_states, value_states, seq_in, sec_in, dia_in)


def attend_kernel(
    info_ref, q_ref, k_ref, v_ref, seq_q, sec_q, dia_q, seq_kv, sec_kv, dia_kv, near_ref,
    own_gate, other_gate, latent_ref, *rest
):
    out_ref, qs, ks, vs = rest[-4:]
    rows = q_ref.shape[1]

    @pl.when(pl.program_id(0) == 0)
    def _():
        lane = lax.broadcasted_iota(jnp.int32, (rows, HEAD_DIM), 1)
        for slot in range(6):
            vs[slot, :, HEAD_DIM:] = (lane == 0).astype(jnp.bfloat16)

    qs[0] = q_ref[0]
    ks[0] = k_ref[0]
    vs[0, :, :HEAD_DIM] = v_ref[0]
    for slot, q_in, kv_in in ((1, seq_q, seq_kv), (2, sec_q, sec_kv), (3, dia_q, dia_kv)):
        qs[slot] = q_in[0]
        ks[slot] = kv_in[0]
        vs[slot, :, :HEAD_DIM] = kv_in[1]
    vs[4, :TAIL, :HEAD_DIM] = near_ref[1]
    vs[5, :TAIL, :HEAD_DIM] = near_ref[3]
    factor = math.log2(math.e) / math.sqrt(HEAD_DIM)
    place = lax.broadcasted_iota(jnp.int32, (1, TAIL), 1)
    bias = jnp.where(place >= info_ref[0], 0.0, -jnp.inf)

    gated = [None, None]
    for layer, gate_ref in enumerate((own_gate, other_gate)):
        keys = (ks[2 * layer], ks[2 * layer + 1], near_ref[2 * layer])
        values = (vs[2 * layer], vs[2 * layer + 1], vs[4 + layer, :TAIL])
        scores = []
        for half in range(2):
            query = qs[2 * layer + half]
            parts = [
                lax.dot_general(
                    query, key, (((1,), (1,)), ((), ())), preferred_element_type=jnp.float32
                )
                for key in keys
            ]
            scores.append(parts[:2] + [parts[2] + bias])
        lifted = []
        for parts in scores:
            top = factor * functools.reduce(
                jnp.maximum, [jnp.max(part, axis=-1, keepdims=True) for part in parts]
            )
            lifted.append([jnp.exp2(part * factor - top).astype(jnp.bfloat16) for part in parts])
        for half, parts in enumerate(lifted):
            mixed = sum(
                jnp.dot(part, value, preferred_element_type=jnp.float32)
                for part, value in zip(parts, values)
            )
            attended = (mixed[:, :HEAD_DIM] / mixed[:, HEAD_DIM : HEAD_DIM + 1]).astype(
                jnp.bfloat16
            )
            term = gate_ref[...] * attended.astype(jnp.float32)
            gated[half] = term if layer == 0 else gated[half] + term
    out_ref[0] = (latent_ref[...].astype(jnp.float32) + gated[0]).astype(jnp.bfloat16)
    out_ref[1] = gated[1].astype(jnp.bfloat16)


def attend(
    info, queries, key_states, value_states, queries_in, pairs_in, near, gate, other_gate,
    latents, first, heads, place, group_heads, filled,
):
    rows = queries.shape[1]
    keys = 2 * rows + TAIL
    local = pl.BlockSpec((1, rows, HEAD_DIM), lambda h, info: (0, 0, info[1] + first + h))
    last = queries_in[0].shape[0] - 1
    operands = [info, queries, key_states, value_states, *queries_in, *pairs_in, near]
    operands += [gate, other_gate, latents]
    in_specs = [local, local, local]
    in_specs += [pl.BlockSpec((1, rows, HEAD_DIM), lambda h, info: (last, 0, h))] * 3
    in_specs += [pl.BlockSpec((2, rows, HEAD_DIM), lambda h, info: (0, 0, h))] * 3
    in_specs.append(pl.BlockSpec((4, TAIL, HEAD_DIM), lambda h, info: (0, 0, h)))
    in_specs.append(pl.BlockSpec((1, HEAD_DIM), lambda h, info: (0, info[1] + first + h)))
    in_specs.append(pl.BlockSpec((1, HEAD_DIM), lambda h, info: (0, first + h)))
    in_specs.append(pl.BlockSpec((rows, HEAD_DIM), lambda h, info: (0, info[1] + first + h)))
    aliases = {}
    if filled is not None:
        aliases = {len(operands): 0}
        operands.append(filled)
        in_specs.append(pl.BlockSpec(memory_space=pl.ANY))
    return pl.pallas_call(
        attend_kernel,
        grid_spec=pltpu.PrefetchScalarGridSpec(
            num_scalar_prefetch=1,
            grid=(heads,),
            in_specs=in_specs,
            out_specs=pl.BlockSpec((2, rows, HEAD_DIM), lambda h, info: (0, 0, place + h)),
            scratch_shapes=[pltpu.VMEM((4, rows, HEAD_DIM), jnp.bfloat16)] * 2
            + [pltpu.VMEM((6, rows, 2 * HEAD_DIM), jnp.bfloat16)],
        ),
        out_shape=jax.ShapeDtypeStruct((2, rows, group_heads * HEAD_DIM), jnp.bfloat16),
        input_output_aliases=aliases,
        cost_estimate=pl.CostEstimate(
            flops=heads * 4 * rows * keys * HEAD_DIM * 4,
            bytes_accessed=heads * HEAD_DIM * rows * 40,
            transcendentals=heads * 4 * rows * keys,
        ),
        compiler_params=pltpu.CompilerParams(vmem_limit_bytes=VMEM_LIMIT),
        name="attend",
    )(*operands)


def tail_rows(summed, far, seq):
    cut = far.shape[0] - TAIL
    mine = lax.dynamic_slice(summed, (1 - seq, cut, 0), (1, TAIL, far.shape[1]))[0]
    whole = mine.astype(jnp.float32) + far[cut:].astype(jnp.float32)
    return jnp.where(seq == 1, mine, whole.astype(jnp.bfloat16))


def finish_kernel(steps, info_ref, *rest):
    out_ref = rest[-1]
    seq, shared = info_ref[3], info_ref[4]

    def fill(summed_ref, far_ref, tail_ref):
        out_ref[seq] = summed_ref[0]
        whole = far_ref[...].astype(jnp.float32) + summed_ref[1].astype(jnp.float32)
        out_ref[1 - seq] = whole.astype(jnp.bfloat16)
        for frame in range(BF):
            source = jnp.clip(BF - shared + frame, 0, BF - 1)
            weight = (info_ref[5 + frame].astype(jnp.float32) + 0.5) / WEIGHTS
            begin = pl.multiple_of(source * TOK_FRAME, TOK_FRAME)
            place = pl.ds(frame * TOK_FRAME, TOK_FRAME)

            @pl.when(frame < shared)
            def _():
                before = tail_ref[pl.ds(begin, TOK_FRAME), :].astype(jnp.float32)
                lead = out_ref[0, place, :].astype(jnp.float32)
                mixed = weight * lead + (1.0 - weight) * before
                out_ref[0, place, :] = mixed.astype(jnp.bfloat16)

    step = pl.program_id(0)
    begin = 0
    for part, count in enumerate(steps):
        refs = rest[3 * part : 3 * part + 3]
        if len(steps) == 1:
            fill(*refs)
        else:
            pl.when((step >= begin) & (step < begin + count))(functools.partial(fill, *refs))
        begin += count


def finish(info, parts, first, second):
    rows = parts[0][0].shape[1]
    width = 2 * HEAD_DIM
    steps = tuple(part[0].shape[2] // width for part in parts)
    operands, in_specs = [info], []
    begin = 0
    for part, count in zip(parts, steps):
        at = lambda h, begin=begin, count=count: jnp.clip(h - begin, 0, count - 1)
        operands += part
        in_specs += [
            pl.BlockSpec((2, rows, width), lambda h, info, at=at: (0, 0, at(h))),
            pl.BlockSpec((rows, width), lambda h, info, at=at: (0, at(h))),
            pl.BlockSpec((TAIL, width), lambda h, info, at=at: (0, at(h))),
        ]
        begin += count
    aliases = {}
    if second is not None:
        aliases = {len(operands): 0}
        operands.append(second)
        in_specs.append(pl.BlockSpec(memory_space=pl.ANY))
    return pl.pallas_call(
        functools.partial(finish_kernel, steps),
        grid_spec=pltpu.PrefetchScalarGridSpec(
            num_scalar_prefetch=1,
            grid=(begin,),
            in_specs=in_specs,
            out_specs=pl.BlockSpec((2, rows, width), lambda h, info: (0, 0, first // 2 + h)),
        ),
        out_shape=jax.ShapeDtypeStruct((2, rows, QUARTER_HEADS * HEAD_DIM), jnp.bfloat16),
        input_output_aliases=aliases,
        cost_estimate=pl.CostEstimate(
            flops=rows * begin * width * 200,
            bytes_accessed=rows * begin * width * 12,
            transcendentals=0,
        ),
        compiler_params=pltpu.CompilerParams(vmem_limit_bytes=VMEM_LIMIT),
        name="finish",
    )(*operands)


def local(
    latents, queries, key_states, value_states, gate_scales, window, intersection, blend_index
):
    rows = latents.shape[0]
    quarter = QUARTER_HEADS * HEAD_DIM
    span_pos = lax.axis_index("span")
    section = lax.axis_index("section")
    seq = lax.axis_index("seq")
    earlier = jnp.maximum(span_pos - 1, 0)
    follows = span_pos > 0
    closed = jnp.where(follows, TAIL - TOK_FRAME * window[earlier], TAIL)
    shared = jnp.where(follows, intersection[earlier], 0)
    info = jnp.stack([closed, spot(section, seq) * QUARTER_HEADS, section, seq, shared])
    info = jnp.concatenate([info, blend_index[earlier]]).astype(jnp.int32)
    far_base = spot(1 - section, 1 - seq) * quarter

    chunks, groups = len(CHUNKS), len(GROUPS)
    starts = [sum(CHUNKS[:i]) for i in range(chunks)]
    group_first = [starts[group[0]] for group in GROUPS]
    group_heads = [sum(CHUNKS[k] for k in group) for group in GROUPS]
    queries_in, pairs_in = {}, {}
    for kind, k in SENDS:
        first, heads = starts[k], CHUNKS[k]
        sources = {"z": (key_states, value_states, queries), "kv": (key_states, value_states),
                   "q": (queries,)}[kind]
        ways = {"dia": (1, 1), "seq": (0, 1), "sec": (1, 0)}
        arrived = {}
        batches = (("dia",), ("seq", "sec")) if (kind, k) == SENDS[0] else (tuple(ways),)
        for batch in batches:
            packed = pack(
                sources, first * HEAD_DIM, heads * HEAD_DIM, tuple(ways[way] for way in batch)
            )
            for way, block in zip(batch, packed):
                arrived[way] = to_partner(block, *ways[way])
        arrived = (arrived["seq"], arrived["sec"], arrived["dia"])
        if kind in ("z", "q"):
            queries_in[k] = arrived
        if kind in ("z", "kv"):
            pairs_in[k] = arrived
    far_latents = []
    for first, heads in zip(group_first, group_heads):
        sent = lax.dynamic_slice_in_dim(
            latents, far_base + first * HEAD_DIM, heads * HEAD_DIM, 1
        )
        far_latents.append(to_partner(sent, 1, 1))
    other_gate = to_partner(
        lax.dynamic_slice_in_dim(gate_scales, spot(1 - section, seq) * quarter, quarter, 1), 1, 0
    )

    attended = []
    for g, group in enumerate(GROUPS):
        filled = None
        for k in group:
            first, heads = starts[k], CHUNKS[k]
            near = near_rows(
                info, key_states, value_states, *pairs_in[k], first * HEAD_DIM,
                heads * HEAD_DIM,
            )
            near = to_next_span(near)
            filled = attend(
                info, queries, key_states, value_states, queries_in[k], pairs_in[k], near,
                gate_scales, other_gate, latents, first, heads, first - group_first[g], group_heads[g], filled,
            )
        attended.append(filled)

    tails = []
    for g in range(groups):
        far = far_latents[g]
        if g:
            far, _ = lax.optimization_barrier((far, tails[-1]))
        tail = tail_rows(attended[g], far, seq)
        tails.append(tail)
    arrived_tails = []
    for g in range(groups):
        arrived_tails.append(to_next_span(tails[g]))
    second = None
    for members in FINISHES:
        parts = [(attended[g], far_latents[g], arrived_tails[g]) for g in members]
        second = finish(info, parts, group_first[members[0]], second)
    return second.reshape(2 * rows, quarter)


def solution(mesh):
    in_specs = (
        P(("span", "seq"), None),
        P("section", ("span", "seq"), None),
        P("section", ("span", "seq"), None),
        P("section", ("span", "seq"), None),
        P("section", None),
        P(),
        P(),
        P(),
    )
    out_specs = P("span", ("section", "seq"))

    return jax.shard_map(local, mesh=mesh, in_specs=in_specs, out_specs=out_specs, check_vma=False)
```

```python
import functools
import math

import jax
import jax.numpy as jnp
from jax import lax
from jax.experimental import pallas as pl
from jax.experimental.pallas import tpu as pltpu
from jax.sharding import PartitionSpec as P


HEAD_DIM = 128
TOK_FRAME = 48
BF = 10
WEIGHTS = 8
TAIL = BF * TOK_FRAME
QUARTER_HEADS = 10
CHUNKS = (3, 3, 2, 2)
GROUPS = ((0, 1), (2,), (3,))
FINISHES = ((0,), (1, 2))
FINISH_HEADS = {1: 3, 2: 2}
SENDS = (("z", 0), ("z", 1), ("kv", 2), ("kv", 3), ("q", 2), ("q", 3))
VMEM_LIMIT = 66000 * 1024
PAIR_AXES = ("section", "seq")


def spot(section, seq):
    return section * 2 + seq


def to_partner(block, flip_section, flip_seq):
    pairs = [
        (spot(s, q), spot(s ^ flip_section, q ^ flip_seq)) for s in range(2) for q in range(2)
    ]
    return lax.ppermute(block, PAIR_AXES, pairs)


def to_next_span(block):
    length = lax.axis_size("span")
    return lax.ppermute(block, "span", [(i, i + 1) for i in range(length - 1)])


def pack_kernel(width, start, dests, count, *rest):
    sources, outs, (stage, in_sems, out_sems) = rest[:count], rest[count:-3], rest[-3:]
    section, seq = lax.axis_index("section"), lax.axis_index("seq")
    copies = []
    for at, (flip_section, flip_seq) in enumerate(dests):
        other_section = 1 - section if flip_section else section
        other_seq = 1 - seq if flip_seq else seq
        col = spot(other_section, other_seq) * QUARTER_HEADS * HEAD_DIM + start
        col = pl.multiple_of(col, HEAD_DIM)
        for which, ref in enumerate(sources):
            taken = pltpu.make_async_copy(
                ref.at[0, :, pl.ds(col, width)], stage.at[at, which], in_sems.at[at, which]
            )
            taken.start()
            copies.append((at, which, taken))
    sent = []
    for at, which, taken in copies:
        taken.wait()
        put = pltpu.make_async_copy(
            stage.at[at, which], outs[at].at[which], out_sems.at[at, which]
        )
        put.start()
        sent.append(put)
    for put in sent:
        put.wait()


def pack(sources, start, width, dests):
    rows, count = sources[0].shape[1], len(sources)
    shape = jax.ShapeDtypeStruct((count, rows, width), jnp.bfloat16)
    return pl.pallas_call(
        functools.partial(pack_kernel, width, start, dests, count),
        in_specs=[pl.BlockSpec(memory_space=pl.ANY)] * count,
        out_specs=[pl.BlockSpec(memory_space=pl.ANY)] * len(dests),
        scratch_shapes=[
            pltpu.VMEM((len(dests), count, rows, width), jnp.bfloat16),
            pltpu.SemaphoreType.DMA((len(dests), count)),
            pltpu.SemaphoreType.DMA((len(dests), count)),
        ],
        out_shape=[shape] * len(dests),
        cost_estimate=pl.CostEstimate(
            flops=count * len(dests) * rows * width * 8,
            bytes_accessed=4 * count * len(dests) * rows * width,
            transcendentals=0,
        ),
        compiler_params=pltpu.CompilerParams(vmem_limit_bytes=VMEM_LIMIT),
        name="pack",
    )(*sources)


def near_kernel(
    width, start, info_ref, k_ref, v_ref, seq_ref, sec_ref, dia_ref, out_ref, stage, sems, out_sems
):
    rows = k_ref.shape[1]
    cut = pl.ds(rows - TAIL, TAIL)
    cols = pl.ds(pl.multiple_of(info_ref[1] * HEAD_DIM + start, HEAD_DIM), width)
    late = info_ref[3] == 1

    @pl.when(late)
    def _():
        pltpu.make_async_copy(k_ref.at[0, cut, cols], stage.at[0], sems.at[0]).start()
        pltpu.make_async_copy(v_ref.at[0, cut, cols], stage.at[1], sems.at[1]).start()
        pltpu.make_async_copy(sec_ref.at[0, cut], stage.at[2], sems.at[2]).start()
        pltpu.make_async_copy(sec_ref.at[1, cut], stage.at[3], sems.at[3]).start()

    @pl.when(jnp.logical_not(late))
    def _():
        pltpu.make_async_copy(seq_ref.at[0, cut], stage.at[0], sems.at[0]).start()
        pltpu.make_async_copy(seq_ref.at[1, cut], stage.at[1], sems.at[1]).start()
        pltpu.make_async_copy(dia_ref.at[0, cut], stage.at[2], sems.at[2]).start()
        pltpu.make_async_copy(dia_ref.at[1, cut], stage.at[3], sems.at[3]).start()

    for slot in range(4):
        pltpu.make_async_copy(seq_ref.at[0, cut], stage.at[slot], sems.at[slot]).wait()
        pltpu.make_async_copy(stage.at[slot], out_ref.at[slot], out_sems.at[slot]).start()
    for slot in range(4):
        pltpu.make_async_copy(stage.at[slot], out_ref.at[slot], out_sems.at[slot]).wait()


def near_rows(info, key_states, value_states, seq_in, sec_in, dia_in, start, width):
    return pl.pallas_call(
        functools.partial(near_kernel, width, start),
        grid_spec=pltpu.PrefetchScalarGridSpec(
            num_scalar_prefetch=1,
            grid=(),
            in_specs=[pl.BlockSpec(memory_space=pl.ANY)] * 5,
            out_specs=pl.BlockSpec(memory_space=pl.ANY),
            scratch_shapes=[
                pltpu.VMEM((4, TAIL, width), jnp.bfloat16),
                pltpu.SemaphoreType.DMA((4,)),
                pltpu.SemaphoreType.DMA((4,)),
            ],
        ),
        out_shape=jax.ShapeDtypeStruct((4, TAIL, width), jnp.bfloat16),
        cost_estimate=pl.CostEstimate(
            flops=4 * TAIL * width * 8, bytes_accessed=16 * TAIL * width, transcendentals=0
        ),
        compiler_params=pltpu.CompilerParams(vmem_limit_bytes=VMEM_LIMIT),
        name="near",
    )(info, key_states, value_states, seq_in, sec_in, dia_in)


def attend_kernel(
    info_ref, q_ref, k_ref, v_ref, seq_q, sec_q, dia_q, seq_kv, sec_kv, dia_kv, near_ref,
    own_gate, other_gate, latent_ref, *rest
):
    out_ref, vs = rest[-2:]
    rows = q_ref.shape[1]

    @pl.when(pl.program_id(0) == 0)
    def _():
        lane = lax.broadcasted_iota(jnp.int32, (rows, HEAD_DIM), 1)
        for slot in range(6):
            vs[slot, :, HEAD_DIM:] = (lane == 0).astype(jnp.bfloat16)

    queries = (q_ref, seq_q, sec_q, dia_q)
    keys_of = (k_ref, seq_kv, sec_kv, dia_kv)
    vs[0, :, :HEAD_DIM] = v_ref[0]
    for slot, kv_in in ((1, seq_kv), (2, sec_kv), (3, dia_kv)):
        vs[slot, :, :HEAD_DIM] = kv_in[1]
    vs[4, :TAIL, :HEAD_DIM] = near_ref[1]
    vs[5, :TAIL, :HEAD_DIM] = near_ref[3]
    factor = math.log2(math.e) / math.sqrt(HEAD_DIM)
    place = lax.broadcasted_iota(jnp.int32, (1, TAIL), 1)
    bias = jnp.where(place >= info_ref[0], 0.0, -jnp.inf)

    gated = [None, None]
    for layer, gate_ref in enumerate((own_gate, other_gate)):
        keys = (keys_of[2 * layer][0], keys_of[2 * layer + 1][0], near_ref[2 * layer])
        values = (vs[2 * layer], vs[2 * layer + 1], vs[4 + layer, :TAIL])
        scores = []
        for half in range(2):
            query = queries[2 * layer + half][0]
            parts = [
                lax.dot_general(
                    query, key, (((1,), (1,)), ((), ())), preferred_element_type=jnp.float32
                )
                for key in keys
            ]
            scores.append(parts[:2] + [parts[2] + bias])
        lifted = []
        for parts in scores:
            top = factor * functools.reduce(
                jnp.maximum, [jnp.max(part, axis=-1, keepdims=True) for part in parts]
            )
            lifted.append([jnp.exp2(part * factor - top).astype(jnp.bfloat16) for part in parts])
        for half, parts in enumerate(lifted):
            mixed = sum(
                jnp.dot(part, value, preferred_element_type=jnp.float32)
                for part, value in zip(parts, values)
            )
            attended = (mixed[:, :HEAD_DIM] / mixed[:, HEAD_DIM : HEAD_DIM + 1]).astype(
                jnp.bfloat16
            )
            term = gate_ref[...] * attended.astype(jnp.float32)
            gated[half] = term if layer == 0 else gated[half] + term
    out_ref[0] = (latent_ref[...].astype(jnp.float32) + gated[0]).astype(jnp.bfloat16)
    out_ref[1] = gated[1].astype(jnp.bfloat16)


def attend(
    info, queries, key_states, value_states, queries_in, pairs_in, near, gate, other_gate,
    latents, first, heads, place, group_heads, filled,
):
    rows = queries.shape[1]
    keys = 2 * rows + TAIL
    local = pl.BlockSpec((1, rows, HEAD_DIM), lambda h, info: (0, 0, info[1] + first + h))
    last = queries_in[0].shape[0] - 1
    operands = [info, queries, key_states, value_states, *queries_in, *pairs_in, near]
    operands += [gate, other_gate, latents]
    in_specs = [local, local, local]
    in_specs += [pl.BlockSpec((1, rows, HEAD_DIM), lambda h, info: (last, 0, h))] * 3
    in_specs += [pl.BlockSpec((2, rows, HEAD_DIM), lambda h, info: (0, 0, h))] * 3
    in_specs.append(pl.BlockSpec((4, TAIL, HEAD_DIM), lambda h, info: (0, 0, h)))
    in_specs.append(pl.BlockSpec((1, HEAD_DIM), lambda h, info: (0, info[1] + first + h)))
    in_specs.append(pl.BlockSpec((1, HEAD_DIM), lambda h, info: (0, first + h)))
    in_specs.append(pl.BlockSpec((rows, HEAD_DIM), lambda h, info: (0, info[1] + first + h)))
    aliases = {}
    if filled is not None:
        aliases = {len(operands): 0}
        operands.append(filled)
        in_specs.append(pl.BlockSpec(memory_space=pl.ANY))
    return pl.pallas_call(
        attend_kernel,
        grid_spec=pltpu.PrefetchScalarGridSpec(
            num_scalar_prefetch=1,
            grid=(heads,),
            in_specs=in_specs,
            out_specs=pl.BlockSpec((2, rows, HEAD_DIM), lambda h, info: (0, 0, place + h)),
            scratch_shapes=[pltpu.VMEM((6, rows, 2 * HEAD_DIM), jnp.bfloat16)],
        ),
        out_shape=jax.ShapeDtypeStruct((2, rows, group_heads * HEAD_DIM), jnp.bfloat16),
        input_output_aliases=aliases,
        cost_estimate=pl.CostEstimate(
            flops=heads * 4 * rows * keys * HEAD_DIM * 4,
            bytes_accessed=heads * HEAD_DIM * rows * 40,
            transcendentals=heads * 4 * rows * keys,
        ),
        compiler_params=pltpu.CompilerParams(vmem_limit_bytes=VMEM_LIMIT if first + heads < QUARTER_HEADS else 62 * 1024 * 1024),
        name="attend",
    )(*operands)


def tail_rows(summed, far, seq):
    cut = far.shape[0] - TAIL
    mine = lax.dynamic_slice(summed, (1 - seq, cut, 0), (1, TAIL, far.shape[1]))[0]
    whole = mine.astype(jnp.float32) + far[cut:].astype(jnp.float32)
    return jnp.where(seq == 1, mine, whole.astype(jnp.bfloat16))


def finish_kernel(steps, info_ref, *rest):
    out_ref = rest[-1]
    seq, shared = info_ref[3], info_ref[4]

    def fill(summed_ref, far_ref, tail_ref):
        out_ref[seq] = summed_ref[0]
        whole = far_ref[...].astype(jnp.float32) + summed_ref[1].astype(jnp.float32)
        out_ref[1 - seq] = whole.astype(jnp.bfloat16)
        for frame in range(BF):
            source = jnp.clip(BF - shared + frame, 0, BF - 1)
            weight = (info_ref[5 + frame].astype(jnp.float32) + 0.5) / WEIGHTS
            begin = pl.multiple_of(source * TOK_FRAME, TOK_FRAME)
            place = pl.ds(frame * TOK_FRAME, TOK_FRAME)

            @pl.when(frame < shared)
            def _():
                before = tail_ref[pl.ds(begin, TOK_FRAME), :].astype(jnp.float32)
                lead = out_ref[0, place, :].astype(jnp.float32)
                mixed = weight * lead + (1.0 - weight) * before
                out_ref[0, place, :] = mixed.astype(jnp.bfloat16)

    step = pl.program_id(0)
    begin = 0
    for part, count in enumerate(steps):
        refs = rest[3 * part : 3 * part + 3]
        if len(steps) == 1:
            fill(*refs)
        else:
            pl.when((step >= begin) & (step < begin + count))(functools.partial(fill, *refs))
        begin += count


def finish(info, parts, first, second):
    rows = parts[0][0].shape[1]
    width = FINISH_HEADS[len(parts)] * HEAD_DIM
    steps = tuple(part[0].shape[2] // width for part in parts)
    operands, in_specs = [info], []
    begin = 0
    for part, count in zip(parts, steps):
        at = lambda h, begin=begin, count=count: jnp.clip(h - begin, 0, count - 1)
        operands += part
        in_specs += [
            pl.BlockSpec((2, rows, width), lambda h, info, at=at: (0, 0, at(h))),
            pl.BlockSpec((rows, width), lambda h, info, at=at: (0, at(h))),
            pl.BlockSpec((TAIL, width), lambda h, info, at=at: (0, at(h))),
        ]
        begin += count
    aliases = {}
    if second is not None:
        aliases = {len(operands): 0}
        operands.append(second)
        in_specs.append(pl.BlockSpec(memory_space=pl.ANY))
    return pl.pallas_call(
        functools.partial(finish_kernel, steps),
        grid_spec=pltpu.PrefetchScalarGridSpec(
            num_scalar_prefetch=1,
            grid=(begin,),
            in_specs=in_specs,
            out_specs=pl.BlockSpec(
                (2, rows, width), lambda h, info: (0, 0, first * HEAD_DIM // width + h)
            ),
        ),
        out_shape=jax.ShapeDtypeStruct((2, rows, QUARTER_HEADS * HEAD_DIM), jnp.bfloat16),
        input_output_aliases=aliases,
        cost_estimate=pl.CostEstimate(
            flops=rows * begin * width * 200,
            bytes_accessed=rows * begin * width * 12,
            transcendentals=0,
        ),
        compiler_params=pltpu.CompilerParams(vmem_limit_bytes=24 * 1024 * 1024),
        name="finish",
    )(*operands)


def local(
    latents, queries, key_states, value_states, gate_scales, window, intersection, blend_index
):
    rows = latents.shape[0]
    quarter = QUARTER_HEADS * HEAD_DIM
    span_pos = lax.axis_index("span")
    section = lax.axis_index("section")
    seq = lax.axis_index("seq")
    earlier = jnp.maximum(span_pos - 1, 0)
    follows = span_pos > 0
    closed = jnp.where(follows, TAIL - TOK_FRAME * window[earlier], TAIL)
    shared = jnp.where(follows, intersection[earlier], 0)
    info = jnp.stack([closed, spot(section, seq) * QUARTER_HEADS, section, seq, shared])
    info = jnp.concatenate([info, blend_index[earlier]]).astype(jnp.int32)
    far_base = spot(1 - section, 1 - seq) * quarter

    chunks, groups = len(CHUNKS), len(GROUPS)
    starts = [sum(CHUNKS[:i]) for i in range(chunks)]
    group_first = [starts[group[0]] for group in GROUPS]
    group_heads = [sum(CHUNKS[k] for k in group) for group in GROUPS]
    queries_in, pairs_in = {}, {}
    for kind, k in SENDS:
        first, heads = starts[k], CHUNKS[k]
        sources = {"z": (key_states, value_states, queries), "kv": (key_states, value_states),
                   "q": (queries,)}[kind]
        ways = {"dia": (1, 1), "seq": (0, 1), "sec": (1, 0)}
        arrived = {}
        batches = (("dia",), ("seq", "sec")) if (kind, k) == SENDS[0] else (tuple(ways),)
        for batch in batches:
            packed = pack(
                sources, first * HEAD_DIM, heads * HEAD_DIM, tuple(ways[way] for way in batch)
            )
            for way, block in zip(batch, packed):
                arrived[way] = to_partner(block, *ways[way])
        arrived = (arrived["seq"], arrived["sec"], arrived["dia"])
        if kind in ("z", "q"):
            queries_in[k] = arrived
        if kind in ("z", "kv"):
            pairs_in[k] = arrived
    far_latents = []
    for first, heads in zip(group_first, group_heads):
        sent = lax.dynamic_slice_in_dim(
            latents, far_base + first * HEAD_DIM, heads * HEAD_DIM, 1
        )
        far_latents.append(to_partner(sent, 1, 1))
    other_gate = to_partner(
        lax.dynamic_slice_in_dim(gate_scales, spot(1 - section, seq) * quarter, quarter, 1), 1, 0
    )

    attended = []
    for g, group in enumerate(GROUPS):
        filled = None
        for k in group:
            first, heads = starts[k], CHUNKS[k]
            near = near_rows(
                info, key_states, value_states, *pairs_in[k], first * HEAD_DIM,
                heads * HEAD_DIM,
            )
            near = to_next_span(near)
            filled = attend(
                info, queries, key_states, value_states, queries_in[k], pairs_in[k], near,
                gate_scales, other_gate, latents, first, heads, first - group_first[g], group_heads[g], filled,
            )
        attended.append(filled)

    tails = []
    for g in range(groups):
        far = far_latents[g]
        if g:
            far, _ = lax.optimization_barrier((far, tails[-1]))
        tail = tail_rows(attended[g], far, seq)
        tails.append(tail)
    arrived_tails = []
    for g in range(groups):
        arrived_tails.append(to_next_span(tails[g]))
    second = None
    for members in FINISHES:
        parts = [(attended[g], far_latents[g], arrived_tails[g]) for g in members]
        second = finish(info, parts, group_first[members[0]], second)
    return second.reshape(2 * rows, quarter)


def solution(mesh):
    in_specs = (
        P(("span", "seq"), None),
        P("section", ("span", "seq"), None),
        P("section", ("span", "seq"), None),
        P("section", ("span", "seq"), None),
        P("section", None),
        P(),
        P(),
        P(),
    )
    out_specs = P("span", ("section", "seq"))

    return jax.shard_map(local, mesh=mesh, in_specs=in_specs, out_specs=out_specs, check_vma=False)
```

```python
import functools
import math

import jax
import jax.numpy as jnp
from jax import lax
from jax.experimental import pallas as pl
from jax.experimental.pallas import tpu as pltpu
from jax.sharding import PartitionSpec as P


HEAD_DIM = 128
TOK_FRAME = 48
BF = 10
WEIGHTS = 8
TAIL = BF * TOK_FRAME
QUARTER_HEADS = 10
CHUNKS = (3, 3, 2, 2)
GROUPS = ((0, 1), (2,), (3,))
FINISHES = ((0,), (1,), (2,))
FINISH_HEADS = {6: 3, 2: 2}
SENDS = (("z", 0), ("z", 1), ("kv", 2), ("kv", 3), ("q", 2), ("q", 3))
VMEM_LIMIT = 66000 * 1024
PAIR_AXES = ("section", "seq")


def spot(section, seq):
    return section * 2 + seq


def to_partner(block, flip_section, flip_seq):
    pairs = [
        (spot(s, q), spot(s ^ flip_section, q ^ flip_seq)) for s in range(2) for q in range(2)
    ]
    return lax.ppermute(block, PAIR_AXES, pairs)


def to_next_span(block):
    length = lax.axis_size("span")
    return lax.ppermute(block, "span", [(i, i + 1) for i in range(length - 1)])


def pack_kernel(width, start, dests, count, *rest):
    sources, outs, (stage, in_sems, out_sems) = rest[:count], rest[count:-3], rest[-3:]
    section, seq = lax.axis_index("section"), lax.axis_index("seq")
    copies = []
    for at, (flip_section, flip_seq) in enumerate(dests):
        other_section = 1 - section if flip_section else section
        other_seq = 1 - seq if flip_seq else seq
        col = spot(other_section, other_seq) * QUARTER_HEADS * HEAD_DIM + start
        col = pl.multiple_of(col, HEAD_DIM)
        for which, ref in enumerate(sources):
            taken = pltpu.make_async_copy(
                ref.at[0, :, pl.ds(col, width)], stage.at[at, which], in_sems.at[at, which]
            )
            taken.start()
            copies.append((at, which, taken))
    sent = []
    for at, which, taken in copies:
        taken.wait()
        put = pltpu.make_async_copy(
            stage.at[at, which], outs[at].at[which], out_sems.at[at, which]
        )
        put.start()
        sent.append(put)
    for put in sent:
        put.wait()


def pack(sources, start, width, dests):
    rows, count = sources[0].shape[1], len(sources)
    shape = jax.ShapeDtypeStruct((count, rows, width), jnp.bfloat16)
    return pl.pallas_call(
        functools.partial(pack_kernel, width, start, dests, count),
        in_specs=[pl.BlockSpec(memory_space=pl.ANY)] * count,
        out_specs=[pl.BlockSpec(memory_space=pl.ANY)] * len(dests),
        scratch_shapes=[
            pltpu.VMEM((len(dests), count, rows, width), jnp.bfloat16),
            pltpu.SemaphoreType.DMA((len(dests), count)),
            pltpu.SemaphoreType.DMA((len(dests), count)),
        ],
        out_shape=[shape] * len(dests),
        cost_estimate=pl.CostEstimate(
            flops=count * len(dests) * rows * width * 8,
            bytes_accessed=4 * count * len(dests) * rows * width,
            transcendentals=0,
        ),
        compiler_params=pltpu.CompilerParams(vmem_limit_bytes=VMEM_LIMIT),
        name="pack",
    )(*sources)


def near_kernel(
    width, start, info_ref, k_ref, v_ref, seq_ref, sec_ref, dia_ref, out_ref, stage, sems, out_sems
):
    rows = k_ref.shape[1]
    cut = pl.ds(rows - TAIL, TAIL)
    cols = pl.ds(pl.multiple_of(info_ref[1] * HEAD_DIM + start, HEAD_DIM), width)
    late = info_ref[3] == 1

    @pl.when(late)
    def _():
        pltpu.make_async_copy(k_ref.at[0, cut, cols], stage.at[0], sems.at[0]).start()
        pltpu.make_async_copy(v_ref.at[0, cut, cols], stage.at[1], sems.at[1]).start()
        pltpu.make_async_copy(sec_ref.at[0, cut], stage.at[2], sems.at[2]).start()
        pltpu.make_async_copy(sec_ref.at[1, cut], stage.at[3], sems.at[3]).start()

    @pl.when(jnp.logical_not(late))
    def _():
        pltpu.make_async_copy(seq_ref.at[0, cut], stage.at[0], sems.at[0]).start()
        pltpu.make_async_copy(seq_ref.at[1, cut], stage.at[1], sems.at[1]).start()
        pltpu.make_async_copy(dia_ref.at[0, cut], stage.at[2], sems.at[2]).start()
        pltpu.make_async_copy(dia_ref.at[1, cut], stage.at[3], sems.at[3]).start()

    for slot in range(4):
        pltpu.make_async_copy(seq_ref.at[0, cut], stage.at[slot], sems.at[slot]).wait()
        pltpu.make_async_copy(stage.at[slot], out_ref.at[slot], out_sems.at[slot]).start()
    for slot in range(4):
        pltpu.make_async_copy(stage.at[slot], out_ref.at[slot], out_sems.at[slot]).wait()


def near_rows(info, key_states, value_states, seq_in, sec_in, dia_in, start, width):
    return pl.pallas_call(
        functools.partial(near_kernel, width, start),
        grid_spec=pltpu.PrefetchScalarGridSpec(
            num_scalar_prefetch=1,
            grid=(),
            in_specs=[pl.BlockSpec(memory_space=pl.ANY)] * 5,
            out_specs=pl.BlockSpec(memory_space=pl.ANY),
            scratch_shapes=[
                pltpu.VMEM((4, TAIL, width), jnp.bfloat16),
                pltpu.SemaphoreType.DMA((4,)),
                pltpu.SemaphoreType.DMA((4,)),
            ],
        ),
        out_shape=jax.ShapeDtypeStruct((4, TAIL, width), jnp.bfloat16),
        cost_estimate=pl.CostEstimate(
            flops=4 * TAIL * width * 8, bytes_accessed=16 * TAIL * width, transcendentals=0
        ),
        compiler_params=pltpu.CompilerParams(vmem_limit_bytes=VMEM_LIMIT),
        name="near",
    )(info, key_states, value_states, seq_in, sec_in, dia_in)


def attend_kernel(
    info_ref, q_ref, k_ref, v_ref, seq_q, sec_q, dia_q, seq_kv, sec_kv, dia_kv, near_ref,
    own_gate, other_gate, latent_ref, *rest
):
    out_ref, vs = rest[-2:]
    rows = q_ref.shape[1]

    @pl.when(pl.program_id(0) == 0)
    def _():
        lane = lax.broadcasted_iota(jnp.int32, (rows, HEAD_DIM), 1)
        for slot in range(6):
            vs[slot, :, HEAD_DIM:] = (lane == 0).astype(jnp.bfloat16)

    queries = (q_ref, seq_q, sec_q, dia_q)
    keys_of = (k_ref, seq_kv, sec_kv, dia_kv)
    vs[0, :, :HEAD_DIM] = v_ref[0]
    for slot, kv_in in ((1, seq_kv), (2, sec_kv), (3, dia_kv)):
        vs[slot, :, :HEAD_DIM] = kv_in[1]
    vs[4, :TAIL, :HEAD_DIM] = near_ref[1]
    vs[5, :TAIL, :HEAD_DIM] = near_ref[3]
    factor = math.log2(math.e) / math.sqrt(HEAD_DIM)
    place = lax.broadcasted_iota(jnp.int32, (1, TAIL), 1)
    bias = jnp.where(place >= info_ref[0], 0.0, -jnp.inf)

    gated = [None, None]
    for layer, gate_ref in enumerate((own_gate, other_gate)):
        keys = (keys_of[2 * layer][0], keys_of[2 * layer + 1][0], near_ref[2 * layer])
        values = (vs[2 * layer], vs[2 * layer + 1], vs[4 + layer, :TAIL])
        scores = []
        for half in range(2):
            query = queries[2 * layer + half][0]
            parts = [
                lax.dot_general(
                    query, key, (((1,), (1,)), ((), ())), preferred_element_type=jnp.float32
                )
                for key in keys
            ]
            scores.append(parts[:2] + [parts[2] + bias])
        lifted = []
        for parts in scores:
            top = factor * functools.reduce(
                jnp.maximum, [jnp.max(part, axis=-1, keepdims=True) for part in parts]
            )
            lifted.append([jnp.exp2(part * factor - top).astype(jnp.bfloat16) for part in parts])
        for half, parts in enumerate(lifted):
            mixed = sum(
                jnp.dot(part, value, preferred_element_type=jnp.float32)
                for part, value in zip(parts, values)
            )
            attended = (mixed[:, :HEAD_DIM] / mixed[:, HEAD_DIM : HEAD_DIM + 1]).astype(
                jnp.bfloat16
            )
            term = gate_ref[...] * attended.astype(jnp.float32)
            gated[half] = term if layer == 0 else gated[half] + term
    out_ref[0] = (latent_ref[...].astype(jnp.float32) + gated[0]).astype(jnp.bfloat16)
    out_ref[1] = gated[1].astype(jnp.bfloat16)


def attend(
    info, queries, key_states, value_states, queries_in, pairs_in, near, gate, other_gate,
    latents, first, heads, place, group_heads, filled,
):
    rows = queries.shape[1]
    keys = 2 * rows + TAIL
    local = pl.BlockSpec((1, rows, HEAD_DIM), lambda h, info: (0, 0, info[1] + first + h))
    last = queries_in[0].shape[0] - 1
    operands = [info, queries, key_states, value_states, *queries_in, *pairs_in, near]
    operands += [gate, other_gate, latents]
    in_specs = [local, local, local]
    in_specs += [pl.BlockSpec((1, rows, HEAD_DIM), lambda h, info: (last, 0, h))] * 3
    in_specs += [pl.BlockSpec((2, rows, HEAD_DIM), lambda h, info: (0, 0, h))] * 3
    in_specs.append(pl.BlockSpec((4, TAIL, HEAD_DIM), lambda h, info: (0, 0, h)))
    in_specs.append(pl.BlockSpec((1, HEAD_DIM), lambda h, info: (0, info[1] + first + h)))
    in_specs.append(pl.BlockSpec((1, HEAD_DIM), lambda h, info: (0, first + h)))
    in_specs.append(pl.BlockSpec((rows, HEAD_DIM), lambda h, info: (0, info[1] + first + h)))
    aliases = {}
    if filled is not None:
        aliases = {len(operands): 0}
        operands.append(filled)
        in_specs.append(pl.BlockSpec(memory_space=pl.ANY))
    return pl.pallas_call(
        attend_kernel,
        grid_spec=pltpu.PrefetchScalarGridSpec(
            num_scalar_prefetch=1,
            grid=(heads,),
            in_specs=in_specs,
            out_specs=pl.BlockSpec((2, rows, HEAD_DIM), lambda h, info: (0, 0, place + h)),
            scratch_shapes=[pltpu.VMEM((6, rows, 2 * HEAD_DIM), jnp.bfloat16)],
        ),
        out_shape=jax.ShapeDtypeStruct((2, rows, group_heads * HEAD_DIM), jnp.bfloat16),
        input_output_aliases=aliases,
        cost_estimate=pl.CostEstimate(
            flops=heads * 4 * rows * keys * HEAD_DIM * 4,
            bytes_accessed=heads * HEAD_DIM * rows * 40,
            transcendentals=heads * 4 * rows * keys,
        ),
        compiler_params=pltpu.CompilerParams(vmem_limit_bytes=VMEM_LIMIT if first + heads < QUARTER_HEADS else 62 * 1024 * 1024),
        name="attend",
    )(*operands)


def tail_rows(summed, far, seq):
    cut = far.shape[0] - TAIL
    mine = lax.dynamic_slice(summed, (1 - seq, cut, 0), (1, TAIL, far.shape[1]))[0]
    whole = mine.astype(jnp.float32) + far[cut:].astype(jnp.float32)
    return jnp.where(seq == 1, mine, whole.astype(jnp.bfloat16))


def finish_kernel(steps, info_ref, *rest):
    out_ref = rest[-1]
    seq, shared = info_ref[3], info_ref[4]

    def fill(summed_ref, far_ref, tail_ref):
        out_ref[seq] = summed_ref[0]
        whole = far_ref[...].astype(jnp.float32) + summed_ref[1].astype(jnp.float32)
        out_ref[1 - seq] = whole.astype(jnp.bfloat16)
        for frame in range(BF):
            source = jnp.clip(BF - shared + frame, 0, BF - 1)
            weight = (info_ref[5 + frame].astype(jnp.float32) + 0.5) / WEIGHTS
            begin = pl.multiple_of(source * TOK_FRAME, TOK_FRAME)
            place = pl.ds(frame * TOK_FRAME, TOK_FRAME)

            @pl.when(frame < shared)
            def _():
                before = tail_ref[pl.ds(begin, TOK_FRAME), :].astype(jnp.float32)
                lead = out_ref[0, place, :].astype(jnp.float32)
                mixed = weight * lead + (1.0 - weight) * before
                out_ref[0, place, :] = mixed.astype(jnp.bfloat16)

    step = pl.program_id(0)
    begin = 0
    for part, count in enumerate(steps):
        refs = rest[3 * part : 3 * part + 3]
        if len(steps) == 1:
            fill(*refs)
        else:
            pl.when((step >= begin) & (step < begin + count))(functools.partial(fill, *refs))
        begin += count


def finish(info, parts, first, second):
    rows = parts[0][0].shape[1]
    width = FINISH_HEADS[parts[0][0].shape[2] // HEAD_DIM] * HEAD_DIM
    steps = tuple(part[0].shape[2] // width for part in parts)
    operands, in_specs = [info], []
    begin = 0
    for part, count in zip(parts, steps):
        at = lambda h, begin=begin, count=count: jnp.clip(h - begin, 0, count - 1)
        operands += part
        in_specs += [
            pl.BlockSpec((2, rows, width), lambda h, info, at=at: (0, 0, at(h))),
            pl.BlockSpec((rows, width), lambda h, info, at=at: (0, at(h))),
            pl.BlockSpec((TAIL, width), lambda h, info, at=at: (0, at(h))),
        ]
        begin += count
    aliases = {}
    if second is not None:
        aliases = {len(operands): 0}
        operands.append(second)
        in_specs.append(pl.BlockSpec(memory_space=pl.ANY))
    return pl.pallas_call(
        functools.partial(finish_kernel, steps),
        grid_spec=pltpu.PrefetchScalarGridSpec(
            num_scalar_prefetch=1,
            grid=(begin,),
            in_specs=in_specs,
            out_specs=pl.BlockSpec(
                (2, rows, width), lambda h, info: (0, 0, first * HEAD_DIM // width + h)
            ),
        ),
        out_shape=jax.ShapeDtypeStruct((2, rows, QUARTER_HEADS * HEAD_DIM), jnp.bfloat16),
        input_output_aliases=aliases,
        cost_estimate=pl.CostEstimate(
            flops=rows * begin * width * 200,
            bytes_accessed=rows * begin * width * 12,
            transcendentals=0,
        ),
        compiler_params=pltpu.CompilerParams(vmem_limit_bytes=24 * 1024 * 1024),
        name="finish",
    )(*operands)


def local(
    latents, queries, key_states, value_states, gate_scales, window, intersection, blend_index
):
    rows = latents.shape[0]
    quarter = QUARTER_HEADS * HEAD_DIM
    span_pos = lax.axis_index("span")
    section = lax.axis_index("section")
    seq = lax.axis_index("seq")
    earlier = jnp.maximum(span_pos - 1, 0)
    follows = span_pos > 0
    closed = jnp.where(follows, TAIL - TOK_FRAME * window[earlier], TAIL)
    shared = jnp.where(follows, intersection[earlier], 0)
    info = jnp.stack([closed, spot(section, seq) * QUARTER_HEADS, section, seq, shared])
    info = jnp.concatenate([info, blend_index[earlier]]).astype(jnp.int32)
    far_base = spot(1 - section, 1 - seq) * quarter

    chunks, groups = len(CHUNKS), len(GROUPS)
    starts = [sum(CHUNKS[:i]) for i in range(chunks)]
    group_first = [starts[group[0]] for group in GROUPS]
    group_heads = [sum(CHUNKS[k] for k in group) for group in GROUPS]
    queries_in, pairs_in = {}, {}
    for kind, k in SENDS:
        first, heads = starts[k], CHUNKS[k]
        sources = {"z": (key_states, value_states, queries), "kv": (key_states, value_states),
                   "q": (queries,)}[kind]
        ways = {"dia": (1, 1), "seq": (0, 1), "sec": (1, 0)}
        arrived = {}
        batches = (("dia",), ("seq", "sec")) if (kind, k) == SENDS[0] else (tuple(ways),)
        for batch in batches:
            packed = pack(
                sources, first * HEAD_DIM, heads * HEAD_DIM, tuple(ways[way] for way in batch)
            )
            for way, block in zip(batch, packed):
                arrived[way] = to_partner(block, *ways[way])
        arrived = (arrived["seq"], arrived["sec"], arrived["dia"])
        if kind in ("z", "q"):
            queries_in[k] = arrived
        if kind in ("z", "kv"):
            pairs_in[k] = arrived
    far_latents = []
    for first, heads in zip(group_first, group_heads):
        sent = lax.dynamic_slice_in_dim(
            latents, far_base + first * HEAD_DIM, heads * HEAD_DIM, 1
        )
        far_latents.append(to_partner(sent, 1, 1))
    other_gate = to_partner(
        lax.dynamic_slice_in_dim(gate_scales, spot(1 - section, seq) * quarter, quarter, 1), 1, 0
    )

    attended = []
    for g, group in enumerate(GROUPS):
        filled = None
        for k in group:
            first, heads = starts[k], CHUNKS[k]
            near = near_rows(
                info, key_states, value_states, *pairs_in[k], first * HEAD_DIM,
                heads * HEAD_DIM,
            )
            near = to_next_span(near)
            filled = attend(
                info, queries, key_states, value_states, queries_in[k], pairs_in[k], near,
                gate_scales, other_gate, latents, first, heads, first - group_first[g], group_heads[g], filled,
            )
        attended.append(filled)

    tails = []
    for g in range(groups):
        far = far_latents[g]
        if g:
            far, _ = lax.optimization_barrier((far, tails[-1]))
        tail = tail_rows(attended[g], far, seq)
        tails.append(tail)
    arrived_tails = []
    for g in range(groups):
        arrived_tails.append(to_next_span(tails[g]))
    second = None
    for members in FINISHES:
        parts = [(attended[g], far_latents[g], arrived_tails[g]) for g in members]
        second = finish(info, parts, group_first[members[0]], second)
    return second.reshape(2 * rows, quarter)


def solution(mesh):
    in_specs = (
        P(("span", "seq"), None),
        P("section", ("span", "seq"), None),
        P("section", ("span", "seq"), None),
        P("section", ("span", "seq"), None),
        P("section", None),
        P(),
        P(),
        P(),
    )
    out_specs = P("span", ("section", "seq"))

    return jax.shard_map(local, mesh=mesh, in_specs=in_specs, out_specs=out_specs, check_vma=False)
```
